256 devices in a mesh: seg: 256 (over x, z, y, core).
Axes of the slice: x: 4, y: 4, z: 8, core: 2. Of those that a mesh axis runs over, the one named last changes fastest.
Arguments:
- cam_jac: bfloat16 [18, 4096, 512], P(None, 'seg'), may hold values from -0.25 to 0.25
- point_jac: bfloat16 [6, 4096, 512], P(None, 'seg'), may hold values from -6 to 6
- obs_point: int32 [4096, 512], P('seg'), may hold values from 0 to 1791, as said below
- obs_count: int32 [4096], P('seg'), may hold values from 64 to 512, as said below
- back_list: int32 [256, 384], P('seg'), may hold values from 0 to 1023, as said below
- front_list: int32 [256, 384], P('seg'), may hold values from 0 to 1023, as said below
- point_damp: float32 [262144], P('seg'), may hold values from 0.5 to 4
- cam_damp: float32 [4096], P('seg'), may hold values from 0.1 to 1
- right_side: float32 [9, 4096], P(None, 'seg'), may hold values from -25 to 25
- start_guess: float32 [9, 4096], P(None, 'seg'), may hold values from -3 to 3
Outputs:
- camera_step: float32 [9, 4096], P(None, 'seg')
- residual: float32 [9, 4096], P(None, 'seg')
The draws below stay inside these ranges and needn't reach their ends.
Inputs may be any that keep to these rules, and one draw needn't show every extreme that they name: `obs_point`: entries below 1024 name the segment's own points; an entry e from 1024 to 1407 names entry e - 1024 of the previous segment's back_list, and a larger one entry e - 1408 of the next segment's front_list. Keyframes of the first segment name no back slot, those of the last segment no front slot. `obs_count`: slots at or past a keyframe's count are padding. Every segment has a keyframe whose slots are all used. `back_list`: each row holds 384 distinct own points of the segment; no point stands on both lists of its segment. `front_list`: each row holds 384 distinct own points of the segment; no point stands on both lists of its segment.
All inputs are finite; a program needn't handle non-finite values.
Results may differ from the reference program's by a relative error of at most 0.0005.
Values sent between devices are 32-bit elements; how exact they have to be, the bound alone decides.
A program may use at most 64 MiB of HBM per device.

```python
import math
import jax
import jax.numpy as jnp
from jax import lax

CAM_DEV = 16
OBS_CAM = 512
P_DEV = 1024
ITERS = 2
BORDER = 384
SEGMENTS = 256
CAMERAS = 4096
POINTS = 262144


def border_lists(key):
    seg_keys = jax.random.split(jax.random.fold_in(key, 11), SEGMENTS)
    orders = jax.vmap(lambda seg_key: jax.random.permutation(seg_key, P_DEV))(seg_keys)
    return (orders[:, :BORDER].astype(jnp.int32), orders[:, BORDER:2 * BORDER].astype(jnp.int32))


def draw_back_list(key, part):
    return border_lists(key)[0]


def draw_front_list(key, part):
    return border_lists(key)[1]


def draw_obs_point(key, part):
    side_key, own_key, slot_key = jax.random.split(jax.random.fold_in(key, 3), 3)
    side_pick = jax.random.randint(side_key, (CAMERAS, OBS_CAM), 0, 4)
    segment = (jnp.arange(CAMERAS, dtype=jnp.int32) // CAM_DEV)[:, None]
    own_pick = jax.random.randint(own_key, (CAMERAS, OBS_CAM), 0, P_DEV)
    slot_pick = jax.random.randint(slot_key, (CAMERAS, OBS_CAM), 0, BORDER)
    back_side = (side_pick == 0) & (segment > 0)
    front_side = (side_pick == 1) & (segment < SEGMENTS - 1)
    result = jnp.where(back_side, P_DEV + slot_pick, jnp.where(front_side, P_DEV + BORDER + slot_pick, own_pick))
    return result.astype(jnp.int32)


def draw_obs_count(key, part):
    high_key, count_key, full_key = jax.random.split(jax.random.fold_in(key, 5), 3)
    high_cap = jax.random.randint(high_key, (SEGMENTS,), OBS_CAM // 2, OBS_CAM + 1)
    high_rows = jnp.repeat(high_cap, CAM_DEV)
    low_rows = high_rows // 4
    counts = jax.random.randint(count_key, (CAMERAS,), low_rows, high_rows + 1)
    full_pos = jnp.repeat(jax.random.randint(full_key, (SEGMENTS,), 0, CAM_DEV), CAM_DEV)
    marked = jnp.arange(CAMERAS, dtype=jnp.int32) % CAM_DEV == full_pos
    return jnp.where(marked, OBS_CAM, counts).astype(jnp.int32)


def draw_right_side(key, part):
    first_key = jax.random.fold_in(jax.random.fold_in(key, 9), 0)
    position = jnp.arange(CAMERAS, dtype=jnp.float32) / CAMERAS
    random_part = jnp.clip(jax.random.normal(first_key, (9, CAMERAS), jnp.float32), -6.0, 6.0)
    rising = 3.0 ** position
    return (random_part * rising[None, :]).astype(jnp.float32)


def steps_of(key, extent, pieces, low, top_value):
    def one(dim, shards_of):
        steps = jax.random.uniform(jax.random.fold_in(jax.random.fold_in(key, 6), dim), (shards_of,), jnp.float32, low / len(pieces), top_value / len(pieces))
        return jnp.repeat(jnp.exp(steps), extent[dim] // shards_of).reshape((-1,) + (1,) * (len(extent) - dim - 1))

    gain = one(*pieces[0])
    for cut in pieces[1:]:
        gain = gain * one(*cut)
    return gain


def scatter_about(rng, shape, width, most, pieces=(), kind=jnp.bfloat16):
    values = width * jax.random.normal(rng, shape, jnp.float32)
    if pieces:
        values = values * steps_of(rng, shape, pieces, -0.22, 0.18)
    return jnp.clip(values, -most, most).astype(kind)


def setup_inputs(seed: int = 0) -> dict:
    arg_keys = jax.random.split(jax.random.key(seed), 11)
    cam_jac = scatter_about(arg_keys[0], (18, CAMERAS, OBS_CAM), OBS_CAM ** -0.5, 0.25, ((1, 256),))
    point_jac = scatter_about(arg_keys[1], (6, CAMERAS, OBS_CAM), 1.0, 6.0, ((1, 256),))
    obs_point = draw_obs_point(jax.random.fold_in(arg_keys[10], 71), 0)
    obs_count = draw_obs_count(jax.random.fold_in(arg_keys[10], 71), 0)
    back_list = draw_back_list(jax.random.fold_in(arg_keys[10], 71), 0)
    front_list = draw_front_list(jax.random.fold_in(arg_keys[10], 71), 0)
    point_damp = jnp.clip(jnp.exp(math.log(4.0) - 2.0794415 * jax.random.uniform(arg_keys[6], (POINTS,), jnp.float32) ** steps_of(arg_keys[6], (POINTS,), ((0, 256),), -0.2, 0.2)), 0.5, 4.0)
    cam_damp = jnp.clip(jnp.exp(math.log(1.0) - 2.3025851 * jax.random.uniform(arg_keys[7], (CAMERAS,), jnp.float32) ** steps_of(arg_keys[7], (CAMERAS,), ((0, 256),), -0.2, 0.2)), 0.1, 1.0)
    right_side = draw_right_side(jax.random.fold_in(arg_keys[10], 71), 0)
    start_guess = scatter_about(arg_keys[9], (9, CAMERAS), 0.5, 3.0, ((1, 256),), jnp.float32)
    return {"cam_jac": cam_jac, "point_jac": point_jac, "obs_point": obs_point, "obs_count": obs_count, "back_list": back_list, "front_list": front_list, "point_damp": point_damp, "cam_damp": cam_damp, "right_side": right_side, "start_guess": start_guess}


ENTRY_PAIRS = ((0, 0), (0, 1), (0, 2), (1, 1), (1, 2), (2, 2))


def slot_weights(obs_count, slot_total):
    positions = lax.broadcasted_iota(jnp.int32, (obs_count.shape[0], slot_total), 1)
    return (positions < obs_count[:, None]).astype(jnp.float32)


def global_points(obs_point, back_list, front_list):
    segment = (jnp.arange(obs_point.shape[0], dtype=jnp.int32) // CAM_DEV)[:, None]
    prev_seg = jnp.clip(segment - 1, 0, SEGMENTS - 1)
    next_seg = jnp.clip(segment + 1, 0, SEGMENTS - 1)
    back_slot = jnp.clip(obs_point - P_DEV, 0, BORDER - 1)
    front_slot = jnp.clip(obs_point - P_DEV - BORDER, 0, BORDER - 1)
    own_global = segment * P_DEV + obs_point
    from_back = prev_seg * P_DEV + back_list[prev_seg, back_slot]
    from_front = next_seg * P_DEV + front_list[next_seg, front_slot]
    result = jnp.where(obs_point < P_DEV, own_global, jnp.where(obs_point < P_DEV + BORDER, from_back, from_front))
    return result.astype(jnp.int32).reshape(-1)


def symmetric_inverse(entries):
    cofactors = [entries[3] * entries[5] - entries[4] * entries[4],
                 entries[2] * entries[4] - entries[1] * entries[5],
                 entries[1] * entries[4] - entries[2] * entries[3],
                 entries[0] * entries[5] - entries[2] * entries[2],
                 entries[1] * entries[2] - entries[0] * entries[4],
                 entries[0] * entries[3] - entries[1] * entries[1]]
    determinant = entries[0] * cofactors[0] + entries[1] * cofactors[1] + entries[2] * cofactors[2]
    return [member / determinant for member in cofactors]


def apply_inverse(inverse, point_sums):
    return [inverse[0] * point_sums[0] + inverse[1] * point_sums[1] + inverse[2] * point_sums[2],
            inverse[1] * point_sums[0] + inverse[3] * point_sums[1] + inverse[4] * point_sums[2],
            inverse[2] * point_sums[0] + inverse[4] * point_sums[1] + inverse[5] * point_sums[2]]


def camera_rows(cam_jac, vector, weights):
    error_rows = []
    for row_index in range(2):
        running = cam_jac[9 * row_index].astype(jnp.float32) * vector[0][:, None]
        for column in range(1, 9):
            running = running + cam_jac[9 * row_index + column].astype(jnp.float32) * vector[column][:, None]
        error_rows.append(running * weights)
    return error_rows


def schur_apply(vector, cam_jac, point_jac, weights, owners, inverse, cam_damp):
    errors = camera_rows(cam_jac, vector, weights)
    point_sums = []
    for column in range(3):
        product = errors[0] * point_jac[column].astype(jnp.float32) + errors[1] * point_jac[3 + column].astype(jnp.float32)
        point_sums.append(jax.ops.segment_sum(product.reshape(-1), owners, num_segments=POINTS))
    values = apply_inverse(inverse, point_sums)
    picked = [member[owners].reshape(weights.shape) for member in values]
    adjusted = []
    for row_index in range(2):
        back_term = picked[0] * point_jac[3 * row_index].astype(jnp.float32)
        back_term = back_term + picked[1] * point_jac[3 * row_index + 1].astype(jnp.float32)
        back_term = back_term + picked[2] * point_jac[3 * row_index + 2].astype(jnp.float32)
        adjusted.append(errors[row_index] - weights * back_term)
    result = []
    for column in range(9):
        running = jnp.sum(cam_jac[column].astype(jnp.float32) * adjusted[0] + cam_jac[9 + column].astype(jnp.float32) * adjusted[1], axis=1)
        result.append(cam_damp * vector[column] + running)
    return jnp.stack(result)


def reference(cam_jac, point_jac, obs_point, obs_count, back_list, front_list, point_damp, cam_damp, right_side, start_guess):
    weights = slot_weights(obs_count, obs_point.shape[1])
    owners = global_points(obs_point, back_list, front_list)
    entries = []
    for lead_index, tail_index in ENTRY_PAIRS:
        product = point_jac[lead_index].astype(jnp.float32) * point_jac[tail_index].astype(jnp.float32)
        product = product + point_jac[3 + lead_index].astype(jnp.float32) * point_jac[3 + tail_index].astype(jnp.float32)
        running = jax.ops.segment_sum((product * weights).reshape(-1), owners, num_segments=POINTS)
        if lead_index == tail_index:
            running = running + point_damp
        entries.append(running)
    inverse = symmetric_inverse(entries)
    diagonal = []
    for column in range(9):
        first_sq = cam_jac[column].astype(jnp.float32) ** 2 + cam_jac[9 + column].astype(jnp.float32) ** 2
        diagonal.append(jnp.sum(first_sq * weights, axis=1) + cam_damp)
    precond = 1.0 / jnp.stack(diagonal)

    def operator(vector):
        return schur_apply(vector, cam_jac, point_jac, weights, owners, inverse, cam_damp)

    solution = start_guess
    residual = right_side - operator(solution)
    scaled = precond * residual
    direction = scaled
    inner_now = jnp.sum(residual * scaled)
    for iteration in range(ITERS):
        image = operator(direction)
        step_size = inner_now / jnp.sum(direction * image)
        solution = solution + step_size * direction
        residual = residual - step_size * image
        if iteration + 1 < ITERS:
            scaled = precond * residual
            inner_next = jnp.sum(residual * scaled)
            direction = scaled + (inner_next / inner_now) * direction
            inner_now = inner_next
    return solution, residual
```

```python
import functools

import jax
import jax.numpy as jnp
from jax import lax
from jax.experimental import pallas as pl
from jax.experimental.pallas import tpu as pltpu
from jax.sharding import PartitionSpec as P

DIMS = (4, 8, 4, 2)
PAIRS = ((0, 0), (0, 1), (0, 2), (1, 1), (1, 2), (2, 2))
F32 = jnp.float32
BF16 = jnp.bfloat16
MESH = pl.DeviceIdType.MESH


def spread(block, rows):
    return jnp.broadcast_to(block, (rows, block.shape[1]))


def lane_pick(row, index):
    return jnp.take_along_axis(row, index, axis=1, mode="promise_in_bounds")


def recip(value):
    first = 1.0 / value
    return first * (2.0 - value * first)


def kernel(
    dims,
    cj_ref,
    pj_ref,
    obs_ref,
    cnt_ref,
    back_ref,
    front_ref,
    damp_ref,
    cdamp_ref,
    rhs_ref,
    guess_ref,
    x_ref,
    r_ref,
    oh_lo,
    oh_hi,
    left,
    pieces,
    err,
    wts,
    table,
    next_out0,
    prev_out0,
    from_prev0,
    from_next0,
    next_out,
    prev_out,
    from_prev,
    from_next,
    red_out,
    red_in,
    ex_send,
    ex_recv,
    red_send,
    red_recv,
):
    nx, nz, ny, nc = dims
    total = nx * nz * ny * nc
    cams, slots = obs_ref.shape
    tiles = slots // 128
    me = lax.axis_index("seg")
    core = lax.rem(me, nc)
    y = lax.rem(me // nc, ny)
    z = lax.rem(me // (nc * ny), nz)
    x = me // (nc * ny * nz)

    def ident(px, pz, py, pc):
        return ((px * nz + pz) * ny + py) * nc + pc

    def plane(step):
        px = lax.rem(x + step // ny, nx)
        py = lax.rem(y + step % ny, ny)
        return ident(px, z, py, core)

    def column(step):
        pz = lax.rem(z + step // nc, nz)
        pc = lax.rem(core + step % nc, nc)
        return ident(x, pz, y, pc)

    plane_size, column_size = nx * ny, nz * nc
    plane_me, column_me = x * ny + y, z * nc + core

    def plane_slot(step):
        return lax.rem(x - step // ny + nx, nx) * ny + lax.rem(y - step % ny + ny, ny)

    def column_slot(step):
        return lax.rem(z - step // nc + nz, nz) * nc + lax.rem(core - step % nc + nc, nc)

    has_next, has_prev = me < total - 1, me > 0

    barrier = pltpu.get_barrier_semaphore()
    for step in range(1, plane_size):
        pl.semaphore_signal(barrier, inc=1, device_id=(plane(step),), device_id_type=MESH)
    for step in range(1, column_size):
        pl.semaphore_signal(barrier, inc=1, device_id=(column(step),), device_id_type=MESH)

    @pl.when(has_next)
    def _():
        pl.semaphore_signal(barrier, inc=1, device_id=(me + 1,), device_id_type=MESH)

    @pl.when(has_prev)
    def _():
        pl.semaphore_signal(barrier, inc=1, device_id=(me - 1,), device_id_type=MESH)

    @pl.when(jnp.logical_not(has_prev))
    def _():
        from_prev0[...] = jnp.zeros_like(from_prev0)
        from_prev[...] = jnp.zeros_like(from_prev)

    @pl.when(jnp.logical_not(has_next))
    def _():
        from_next0[...] = jnp.zeros_like(from_next0)
        from_next[...] = jnp.zeros_like(from_next)

    def border_copies(index, to_next, to_prev, came_prev, came_next):
        ahead = pltpu.make_async_remote_copy(
            src_ref=to_next,
            dst_ref=came_prev,
            send_sem=ex_send.at[index, 0],
            recv_sem=ex_recv.at[index, 0],
            device_id=(jnp.minimum(me + 1, total - 1),),
            device_id_type=MESH,
        )
        behind = pltpu.make_async_remote_copy(
            src_ref=to_prev,
            dst_ref=came_next,
            send_sem=ex_send.at[index, 1],
            recv_sem=ex_recv.at[index, 1],
            device_id=(jnp.maximum(me - 1, 0),),
            device_id_type=MESH,
        )
        return ahead, behind

    def border_start(copies):
        ahead, behind = copies

        @pl.when(has_next)
        def _():
            ahead.start()

        @pl.when(has_prev)
        def _():
            behind.start()

    def border_wait(copies):
        ahead, behind = copies

        @pl.when(has_prev)
        def _():
            ahead.wait_recv()
            behind.wait_send()

        @pl.when(has_next)
        def _():
            behind.wait_recv()
            ahead.wait_send()

    def group_copies(stage, size, mine, peer, slot):
        sends = []
        for step in range(1, size):
            sends.append(
                pltpu.make_async_remote_copy(
                    src_ref=red_out.at[stage],
                    dst_ref=red_in.at[stage, mine],
                    send_sem=red_send.at[stage, step - 1],
                    recv_sem=red_recv.at[stage, step - 1],
                    device_id=(peer(step),),
                    device_id_type=MESH,
                )
            )
        waits = []
        for step in range(1, size):
            waits.append(
                pltpu.make_async_remote_copy(
                    src_ref=red_out.at[stage],
                    dst_ref=red_in.at[stage, slot(step)],
                    send_sem=red_send.at[stage, step - 1],
                    recv_sem=red_recv.at[stage, step - 1],
                    device_id=(peer(step),),
                    device_id_type=MESH,
                )
            )
        return sends, waits

    def group_start(stage, value, size, mine, peer, slot):
        sends, waits = group_copies(stage, size, mine, peer, slot)
        red_out[stage] = value
        red_in[stage, mine] = value
        for copy in sends:
            copy.start()
        return sends, waits

    def group_finish(stage, copies, size):
        sends, waits = copies
        for copy in waits:
            copy.wait_recv()
        for copy in sends:
            copy.wait_send()
        result = red_in[stage, 0]
        for step in range(1, size):
            result = result + red_in[stage, step]
        return result

    plane_args = (plane_size, plane_me, plane, plane_slot)
    column_args = (column_size, column_me, column, column_slot)

    eye = lax.broadcasted_iota(jnp.int32, (cams, cams), 0) == lax.broadcasted_iota(
        jnp.int32, (cams, cams), 1
    )

    def stand(row):
        summed = jnp.sum(jnp.where(eye, spread(row, cams), 0.0), axis=1, keepdims=True)
        return jnp.broadcast_to(summed, (cams, 128))

    eye_wide = lax.broadcasted_iota(jnp.int32, (cams, 128), 0) == lax.broadcasted_iota(
        jnp.int32, (cams, 128), 1
    )

    def lie(block):
        return jnp.sum(jnp.where(eye_wide, block, 0.0), axis=0, keepdims=True)[:, :cams]

    def wide(block):
        return jnp.concatenate([block] * tiles, axis=1)

    def stack(block):
        return jnp.concatenate(
            [block[:, 128 * t : 128 * (t + 1)] for t in range(tiles)], axis=0
        )

    def narrow_sum(block):
        summed = jnp.sum(block, axis=1, keepdims=True)
        return jnp.broadcast_to(summed, (cams, 128))

    def inner(first, second):
        running = first[0] * second[0]
        for k in range(1, 9):
            running = running + first[k] * second[k]
        return jnp.sum(running, axis=0, keepdims=True)

    count = stand(cnt_ref[...].astype(F32))
    cam_damp = stand(cdamp_ref[...])
    guess = [stand(guess_ref[k : k + 1, :]) for k in range(9)]
    right = [stand(rhs_ref[k : k + 1, :]) for k in range(9)]
    position = lax.broadcasted_iota(jnp.int32, (cams, slots), 1).astype(F32)
    wts[...] = jnp.where(position < wide(count), 1.0, 0.0)

    lo_line = lax.broadcasted_iota(jnp.int32, (128, slots), 0).astype(F32).astype(BF16)
    hi_line = lax.broadcasted_iota(jnp.int32, (16, slots), 0).astype(F32).astype(BF16)
    one, none = jnp.ones((), BF16), jnp.zeros((), BF16)
    for c in range(cams):
        row = obs_ref[c : c + 1, :]
        low = (row & 127).astype(F32)
        high = (row >> 7).astype(F32)
        here = pl.ds(c * slots, slots)
        oh_lo[:, here] = jnp.where(spread(low, 128).astype(BF16) == lo_line, one, none)
        oh_hi[:, here] = jnp.where(spread(high, 16).astype(BF16) == hi_line, one, none)

    def scatter(groups):
        for c in range(cams):
            here = pl.ds(c * slots, slots)
            mask = oh_hi[:, here]
            for g in range(groups):
                row = spread(pieces[g, c : c + 1, :], 16).astype(BF16)
                left[16 * g : 16 * (g + 1), here] = row * mask
        return lax.dot_general(
            left[: 16 * groups, :],
            oh_lo[...],
            (((1,), (1,)), ((), ())),
            preferred_element_type=F32,
        )

    def cut(index, value):
        first = value.astype(BF16).astype(F32)
        pieces[2 * index] = first
        pieces[2 * index + 1] = value - first

    def joined(result, index):
        return result[32 * index : 32 * index + 16] + result[32 * index + 16 : 32 * index + 32]

    def project(vector):
        weights = wts[...]
        for row in range(2):
            running = cj_ref[9 * row].astype(F32) * wide(vector[0])
            for k in range(1, 9):
                running = running + cj_ref[9 * row + k].astype(F32) * wide(vector[k])
            err[row] = running * weights
        return err[0], err[1]

    def products(base, errors):
        for column_index in range(3):
            cut(
                base + column_index,
                errors[0] * pj_ref[column_index].astype(F32)
                + errors[1] * pj_ref[3 + column_index].astype(F32),
            )

    rows = [back_ref[:, 128 * t : 128 * (t + 1)] for t in range(3)]
    rows += [front_ref[:, 128 * t : 128 * (t + 1)] for t in range(3)]
    rows += [jnp.zeros((2, 128), jnp.int32)]
    listed = jnp.concatenate(rows, axis=0)
    list_lo, list_hi = listed & 127, listed >> 7
    flat = jnp.concatenate([back_ref[...], front_ref[...]], axis=1)
    width = flat.shape[1]
    flat_lo = spread((flat & 127).astype(F32), 128)
    flat_hi = spread((flat >> 7).astype(F32), 8)
    order = lax.broadcasted_iota(jnp.int32, (8, width), 1)
    hot_lo = jnp.where(
        flat_lo == lax.broadcasted_iota(jnp.int32, (128, width), 0).astype(F32), 1.0, 0.0
    ).astype(BF16)
    same_hi = flat_hi == lax.broadcasted_iota(jnp.int32, (8, width), 0).astype(F32)
    marks = jnp.concatenate(
        [
            jnp.where(same_hi, (order & 127).astype(F32), 0.0),
            jnp.where(same_hi, ((order >> 7) + 1).astype(F32), 0.0),
        ],
        axis=0,
    ).astype(BF16)
    places = lax.dot_general(
        marks, hot_lo, (((1,), (1,)), ((), ())), preferred_element_type=F32
    ).astype(jnp.int32)
    place_lo, place_hi = places[:8], places[8:16] - 1

    sub8 = lax.broadcasted_iota(jnp.int32, (8, 128), 0)
    back_rows = sub8 < 3

    def outgoing(sums, index, to_next, to_prev):
        own, outer = sums[:8], sums[8:16]
        picked = jnp.zeros((8, 128), F32)
        for h in range(8):
            found = lane_pick(spread(own[h : h + 1], 8), list_lo)
            picked = jnp.where(list_hi == h, found, picked)
        to_next[index] = jnp.where(back_rows, picked, outer)
        to_prev[index] = jnp.where(back_rows, outer, picked)

    def complete(sums, prev_block, next_block):
        own, outer = sums[:8], sums[8:16]
        mixed = jnp.where(back_rows, next_block, prev_block)
        added = jnp.zeros((8, 128), F32)
        for h in range(6):
            found = lane_pick(spread(mixed[h : h + 1], 8), place_lo)
            added = jnp.where(place_hi == h, found, added)
        return jnp.concatenate(
            [own + added, outer + jnp.where(back_rows, prev_block, next_block)], axis=0
        )

    obs_lo, obs_hi = stack(obs_ref[...] & 127), stack(obs_ref[...] >> 7)

    def finish(vector, errors, sums, inverse):
        points = [
            inverse[0] * sums[0] + inverse[1] * sums[1] + inverse[2] * sums[2],
            inverse[1] * sums[0] + inverse[3] * sums[1] + inverse[4] * sums[2],
            inverse[2] * sums[0] + inverse[4] * sums[1] + inverse[5] * sums[2],
        ]
        for j in range(3):
            table[j] = points[j]
        picked = []
        for j in range(3):
            found = jnp.zeros((cams * tiles, 128), F32)
            for h in range(14):
                row = spread(table[j, h : h + 1, :], cams * tiles)
                found = jnp.where(obs_hi == h, lane_pick(row, obs_lo), found)
            picked.append(
                jnp.concatenate(
                    [found[cams * t : cams * (t + 1)] for t in range(tiles)], axis=1
                )
            )
        weights = wts[...]
        adjusted = []
        for row in range(2):
            term = picked[0] * pj_ref[3 * row].astype(F32)
            term = term + picked[1] * pj_ref[3 * row + 1].astype(F32)
            term = term + picked[2] * pj_ref[3 * row + 2].astype(F32)
            adjusted.append(errors[row] - weights * term)
        image = []
        for k in range(9):
            both = (
                cj_ref[k].astype(F32) * adjusted[0] + cj_ref[9 + k].astype(F32) * adjusted[1]
            )
            image.append(cam_damp * vector[k] + narrow_sum(both))
        return image

    errors = project(guess)
    weights = wts[...]
    for i, (a, b) in enumerate(PAIRS):
        product = pj_ref[a].astype(F32) * pj_ref[b].astype(F32)
        product = product + pj_ref[3 + a].astype(F32) * pj_ref[3 + b].astype(F32)
        cut(i, product * weights)
    products(6, errors)
    result = scatter(18)
    sums = []
    damping = jnp.concatenate([damp_ref[...], jnp.zeros((8, 128), F32)], axis=0)
    for i in range(9):
        value = joined(result, i)
        if i < 6 and PAIRS[i][0] == PAIRS[i][1]:
            value = value + damping
        outgoing(value, i, next_out0, prev_out0)
        sums.append(value)
    pl.semaphore_wait(
        barrier,
        plane_size + column_size - 2 + has_next.astype(jnp.int32) + has_prev.astype(jnp.int32),
    )
    copies = border_copies(0, next_out0, prev_out0, from_prev0, from_next0)
    border_start(copies)
    precond = []
    for k in range(9):
        square = cj_ref[k].astype(F32) ** 2 + cj_ref[9 + k].astype(F32) ** 2
        precond.append(recip(cam_damp + narrow_sum(square * weights)))
    border_wait(copies)
    sums = [complete(sums[i], from_prev0[i], from_next0[i]) for i in range(9)]
    ent = sums[:6]
    cofactors = [
        ent[3] * ent[5] - ent[4] * ent[4],
        ent[2] * ent[4] - ent[1] * ent[5],
        ent[1] * ent[4] - ent[2] * ent[3],
        ent[0] * ent[5] - ent[2] * ent[2],
        ent[1] * ent[2] - ent[0] * ent[4],
        ent[0] * ent[3] - ent[1] * ent[1],
    ]
    determinant = ent[0] * cofactors[0] + ent[1] * cofactors[1] + ent[2] * cofactors[2]
    scale = recip(jnp.where(determinant > 0.0, determinant, 1.0))
    inverse = [member * scale for member in cofactors]
    image = finish(guess, errors, sums[6:], inverse)
    res0 = [right[k] - image[k] for k in range(9)]
    dir0 = [precond[k] * res0[k] for k in range(9)]

    def forward(vector, index):
        errors = project(vector)
        products(0, errors)
        result = scatter(6)
        sums = [joined(result, i) for i in range(3)]
        to_next, to_prev = next_out.at[index], prev_out.at[index]
        for i in range(3):
            outgoing(sums[i], i, to_next, to_prev)
        copies = border_copies(
            1 + index, to_next, to_prev, from_prev.at[index], from_next.at[index]
        )
        border_start(copies)
        return errors, sums, copies

    def backward(vector, index, errors, sums):
        sums = [complete(sums[i], from_prev[index, i], from_next[index, i]) for i in range(3)]
        return finish(vector, errors, sums, inverse)

    lane = lax.broadcasted_iota(jnp.int32, (1, 128), 1)

    def pack(first, second):
        return jnp.where(lane == 0, first, second)

    def unpack(row):
        first = jnp.sum(jnp.where(lane == 0, row, 0.0), axis=1, keepdims=True)
        second = jnp.sum(jnp.where(lane == 1, row, 0.0), axis=1, keepdims=True)
        return jnp.broadcast_to(first, (1, 128)), jnp.broadcast_to(second, (1, 128))

    errors, sums, copies = forward(dir0, 0)
    border_wait(copies)
    img0 = backward(dir0, 0, errors, sums)
    scaled = [precond[k] * img0[k] for k in range(9)]
    reducing = group_start(0, pack(inner(res0, dir0), inner(dir0, img0)), *plane_args)
    errors, sums, copies = forward(scaled, 1)
    value = group_finish(0, reducing, plane_size)
    reducing = group_start(1, value, *column_args)
    border_wait(copies)
    lift = backward(scaled, 1, errors, sums)
    inner0, curve0 = unpack(group_finish(1, reducing, column_size))
    step0 = inner0 * recip(curve0)
    res1 = [res0[k] - step0 * img0[k] for k in range(9)]
    dir1 = [dir0[k] - step0 * scaled[k] for k in range(9)]
    img1 = [img0[k] - step0 * lift[k] for k in range(9)]
    reducing = group_start(2, pack(inner(res1, dir1), inner(dir1, img1)), *plane_args)
    value = group_finish(2, reducing, plane_size)
    reducing = group_start(3, value, *column_args)
    inner1, curve1 = unpack(group_finish(3, reducing, column_size))
    ratio = inner1 * recip(inner0)
    step1 = inner1 * recip(curve1 - ratio * inner1 * recip(step0))
    for k in range(9):
        moved = guess[k] + step0 * dir0[k] + step1 * (dir1[k] + ratio * dir0[k])
        x_ref[k : k + 1, :] = lie(moved)
        left_over = res1[k] - step1 * (img1[k] + ratio * img0[k])
        r_ref[k : k + 1, :] = lie(left_over)


def local(dims, cam_jac, point_jac, obs_point, obs_count, back_list, front_list, point_damp,
          cam_damp, right_side, start_guess):
    cams, slots = obs_point.shape
    entries = cams * slots
    nx, nz, ny, nc = dims
    group = max(nx * ny, nz * nc)
    vmem = pl.BlockSpec(memory_space=pltpu.VMEM)
    shape = jax.ShapeDtypeStruct(right_side.shape, F32)
    return pl.pallas_call(
        functools.partial(kernel, dims),
        out_shape=(shape, shape),
        in_specs=[vmem] * 10,
        out_specs=(vmem, vmem),
        scratch_shapes=[
            pltpu.VMEM((128, entries), BF16),
            pltpu.VMEM((16, entries), BF16),
            pltpu.VMEM((288, entries), BF16),
            pltpu.VMEM((18, cams, slots), F32),
            pltpu.VMEM((2, cams, slots), F32),
            pltpu.VMEM((cams, slots), F32),
            pltpu.VMEM((3, 16, 128), F32),
            pltpu.VMEM((9, 8, 128), F32),
            pltpu.VMEM((9, 8, 128), F32),
            pltpu.VMEM((9, 8, 128), F32),
            pltpu.VMEM((9, 8, 128), F32),
            pltpu.VMEM((2, 3, 8, 128), F32),
            pltpu.VMEM((2, 3, 8, 128), F32),
            pltpu.VMEM((2, 3, 8, 128), F32),
            pltpu.VMEM((2, 3, 8, 128), F32),
            pltpu.VMEM((4, 1, 128), F32),
            pltpu.VMEM((4, group, 1, 128), F32),
            pltpu.SemaphoreType.DMA((3, 2)),
            pltpu.SemaphoreType.DMA((3, 2)),
            pltpu.SemaphoreType.DMA((4, group - 1)),
            pltpu.SemaphoreType.DMA((4, group - 1)),
        ],
        compiler_params=pltpu.CompilerParams(
            collective_id=0, has_side_effects=True, vmem_limit_bytes=48 * 1024 * 1024
        ),
    )(
        cam_jac,
        point_jac,
        obs_point,
        obs_count.reshape(1, cams),
        back_list,
        front_list,
        point_damp.reshape(8, 128),
        cam_damp.reshape(1, cams),
        right_side,
        start_guess,
    )


def solution(mesh):
    seg = "seg"
    return jax.shard_map(
        functools.partial(local, DIMS),
        mesh=mesh,
        in_specs=(
            P(None, seg, None),
            P(None, seg, None),
            P(seg, None),
            P(seg),
            P(seg, None),
            P(seg, None),
            P(seg),
            P(seg),
            P(None, seg),
            P(None, seg),
        ),
        out_specs=(P(None, seg), P(None, seg)),
        check_vma=False,
    )
```

```python
import functools

import jax
import jax.numpy as jnp
from jax import lax
from jax.experimental import pallas as pl
from jax.experimental.pallas import tpu as pltpu
from jax.sharding import PartitionSpec as P

DIMS = (4, 8, 4, 2)
HUB = 1
PAIRS = ((0, 0), (0, 1), (0, 2), (1, 1), (1, 2), (2, 2))
F32 = jnp.float32
BF16 = jnp.bfloat16
MESH = pl.DeviceIdType.MESH


def spread(block, rows):
    return jnp.broadcast_to(block, (rows, block.shape[1]))


def lane_pick(row, index):
    return jnp.take_along_axis(row, index, axis=1, mode="promise_in_bounds")


def recip(value):
    first = 1.0 / value
    return first * (2.0 - value * first)


def kernel(
    dims,
    cj_hbm,
    pj_hbm,
    obs_hbm,
    cnt_hbm,
    back_hbm,
    front_hbm,
    damp_hbm,
    cdamp_hbm,
    rhs_hbm,
    guess_hbm,
    out_ref,
    cj_ref,
    pj_ref,
    obs_ref,
    cnt_ref,
    back_ref,
    front_ref,
    damp_ref,
    cdamp_ref,
    rhs_ref,
    guess_ref,
    load_sem,
    oh_lo,
    oh_hi,
    left,
    pieces,
    err,
    wts,
    table,
    next_out0,
    prev_out0,
    from_prev0,
    from_next0,
    next_out,
    prev_out,
    from_prev,
    from_next,
    first_out,
    first_in,
    second_out,
    second_in,
    ex_send,
    ex_recv,
    first_send,
    first_recv,
    second_send,
    second_recv,
):
    nx, nz, ny, nc = dims
    total = nx * nz * ny * nc
    arrivals = [
        (obs_hbm, obs_ref),
        (cnt_hbm, cnt_ref),
        (guess_hbm, guess_ref),
        (back_hbm, back_ref),
        (front_hbm, front_ref),
        (pj_hbm, pj_ref),
        (cj_hbm, cj_ref),
        (damp_hbm, damp_ref),
        (cdamp_hbm, cdamp_ref),
        (rhs_hbm, rhs_ref),
    ]
    loads = [
        pltpu.make_async_copy(source, target, load_sem.at[i])
        for i, (source, target) in enumerate(arrivals)
    ]
    for load in loads:
        load.start()
    cams, slots = obs_ref.shape
    tiles = slots // 128
    me = lax.axis_index("seg")
    core = lax.rem(me, nc)
    y = lax.rem(me // nc, ny)
    z = lax.rem(me // (nc * ny), nz)
    x = me // (nc * ny * nz)

    def ident(px, pz, py, pc):
        return ((px * nz + pz) * ny + py) * nc + pc

    plane_size = nx * ny
    hub = core == HUB

    def plane_at(step, sign):
        px = lax.rem(x + (step // ny if sign > 0 else nx - step // ny), nx)
        py = lax.rem(y + (step % ny if sign > 0 else ny - step % ny), ny)
        return px, py

    def height_at(step, sign):
        return lax.rem(z + (step if sign > 0 else nz - step), nz)

    has_next, has_prev = me < total - 1, me > 0

    barrier = pltpu.get_barrier_semaphore()

    def greet(device):
        pl.semaphore_signal(barrier, inc=1, device_id=(device,), device_id_type=MESH)

    @pl.when(hub)
    def _():
        for step in range(plane_size):
            px, py = plane_at(step, -1)
            for pc in range(nc):
                if step or pc != HUB:
                    greet(ident(px, z, py, pc))

    for step in range(1, nz):
        greet(ident(x, height_at(step, -1), y, HUB))

    @pl.when(jnp.logical_not(hub))
    def _():
        greet(ident(x, z, y, HUB))

    @pl.when(has_next)
    def _():
        pl.semaphore_signal(barrier, inc=1, device_id=(me + 1,), device_id_type=MESH)

    @pl.when(has_prev)
    def _():
        pl.semaphore_signal(barrier, inc=1, device_id=(me - 1,), device_id_type=MESH)

    @pl.when(jnp.logical_not(has_prev))
    def _():
        from_prev0[...] = jnp.zeros_like(from_prev0)
        from_prev[...] = jnp.zeros_like(from_prev)

    @pl.when(jnp.logical_not(has_next))
    def _():
        from_next0[...] = jnp.zeros_like(from_next0)
        from_next[...] = jnp.zeros_like(from_next)

    def border_copies(index, to_next, to_prev, came_prev, came_next):
        ahead = pltpu.make_async_remote_copy(
            src_ref=to_next,
            dst_ref=came_prev,
            send_sem=ex_send.at[index, 0],
            recv_sem=ex_recv.at[index, 0],
            device_id=(jnp.minimum(me + 1, total - 1),),
            device_id_type=MESH,
        )
        behind = pltpu.make_async_remote_copy(
            src_ref=to_prev,
            dst_ref=came_next,
            send_sem=ex_send.at[index, 1],
            recv_sem=ex_recv.at[index, 1],
            device_id=(jnp.maximum(me - 1, 0),),
            device_id_type=MESH,
        )
        return ahead, behind

    def border_start(copies):
        ahead, behind = copies

        @pl.when(has_next)
        def _():
            ahead.start()

        @pl.when(has_prev)
        def _():
            behind.start()

    def border_wait(copies):
        ahead, behind = copies

        @pl.when(has_prev)
        def _():
            ahead.wait_recv()
            behind.wait_send()

        @pl.when(has_next)
        def _():
            behind.wait_recv()
            ahead.wait_send()

    plane_me = (x * ny + y) * nc + core

    def first_copy(step, sender_core, slot):
        px, py = plane_at(step, 1)
        return pltpu.make_async_remote_copy(
            src_ref=first_out,
            dst_ref=first_in.at[slot],
            send_sem=first_send.at[step],
            recv_sem=first_recv.at[step * nc + sender_core],
            device_id=(ident(px, z, py, HUB),),
            device_id_type=MESH,
        )

    def second_copy(step, pc, slot):
        return pltpu.make_async_remote_copy(
            src_ref=second_out,
            dst_ref=second_in.at[slot],
            send_sem=second_send.at[step * nc + pc],
            recv_sem=second_recv.at[step],
            device_id=(ident(x, height_at(step, 1), y, pc),),
            device_id_type=MESH,
        )

    far_first = sorted(
        range(1, plane_size),
        key=lambda step: -(
            min(step // ny, nx - step // ny) + min(step % ny, ny - step % ny)
        ),
    )
    high_first = sorted(range(1, nz), key=lambda step: -min(step, nz - step))

    def reduce_start(value):
        first_out[...] = value
        for step in far_first:
            first_copy(step, core, plane_me).start()

        @pl.when(hub)
        def _():
            first_in[plane_me] = value

        @pl.when(jnp.logical_not(hub))
        def _():
            first_copy(0, core, plane_me).start()

    def reduce_finish():
        @pl.when(hub)
        def _():
            for step in range(plane_size):
                px, py = plane_at(step, -1)
                for pc in range(nc):
                    if step or pc != HUB:
                        first_copy(step, pc, (px * ny + py) * nc + pc).wait_recv()
            value = first_in[0]
            for slot in range(1, plane_size * nc):
                value = value + first_in[slot]
            second_out[...] = value
            second_in[z] = value
            for step in high_first:
                for pc in range(nc):
                    second_copy(step, pc, z).start()
            for pc in range(nc):
                if pc != HUB:
                    second_copy(0, pc, z).start()

        for step in far_first:
            first_copy(step, core, plane_me).wait_send()

        @pl.when(jnp.logical_not(hub))
        def _():
            first_copy(0, core, plane_me).wait_send()
            second_copy(0, core, z).wait_recv()

        for step in range(1, nz):
            second_copy(step, core, height_at(step, -1)).wait_recv()

        @pl.when(hub)
        def _():
            for step in high_first:
                for pc in range(nc):
                    second_copy(step, pc, z).wait_send()
            for pc in range(nc):
                if pc != HUB:
                    second_copy(0, pc, z).wait_send()

        value = second_in[0]
        for slot in range(1, nz):
            value = value + second_in[slot]
        return value

    eye = lax.broadcasted_iota(jnp.int32, (cams, cams), 0) == lax.broadcasted_iota(
        jnp.int32, (cams, cams), 1
    )

    def stand(row):
        summed = jnp.sum(jnp.where(eye, spread(row, cams), 0.0), axis=1, keepdims=True)
        return jnp.broadcast_to(summed, (cams, 128))

    eye_wide = lax.broadcasted_iota(jnp.int32, (cams, 128), 0) == lax.broadcasted_iota(
        jnp.int32, (cams, 128), 1
    )

    def lie(block):
        return jnp.sum(jnp.where(eye_wide, block, 0.0), axis=0, keepdims=True)[:, :cams]

    def wide(block):
        return jnp.concatenate([block] * tiles, axis=1)

    def stack(block):
        return jnp.concatenate(
            [block[:, 128 * t : 128 * (t + 1)] for t in range(tiles)], axis=0
        )

    def narrow_sum(block):
        summed = jnp.sum(block, axis=1, keepdims=True)
        return jnp.broadcast_to(summed, (cams, 128))

    def inner(first, second):
        running = first[0] * second[0]
        for k in range(1, 9):
            running = running + first[k] * second[k]
        return jnp.sum(running, axis=0, keepdims=True)

    for load in loads[:5]:
        load.wait()
    count = stand(cnt_ref[...].astype(F32))
    guess = [stand(guess_ref[k : k + 1, :]) for k in range(9)]
    position = lax.broadcasted_iota(jnp.int32, (cams, slots), 1).astype(F32)
    wts[...] = jnp.where(position < wide(count), 1.0, 0.0)

    lo_line = lax.broadcasted_iota(jnp.int32, (128, slots), 0).astype(F32).astype(BF16)
    hi_line = lax.broadcasted_iota(jnp.int32, (16, slots), 0).astype(F32).astype(BF16)
    one, none = jnp.ones((), BF16), jnp.zeros((), BF16)
    for c in range(cams):
        row = obs_ref[c : c + 1, :]
        low = (row & 127).astype(F32)
        high = (row >> 7).astype(F32)
        here = pl.ds(c * slots, slots)
        oh_lo[:, here] = jnp.where(spread(low, 128).astype(BF16) == lo_line, one, none)
        oh_hi[:, here] = jnp.where(spread(high, 16).astype(BF16) == hi_line, one, none)

    def scatter(groups):
        for c in range(cams):
            here = pl.ds(c * slots, slots)
            mask = oh_hi[:, here]
            for g in range(groups):
                row = spread(pieces[g, c : c + 1, :], 16).astype(BF16)
                left[16 * g : 16 * (g + 1), here] = row * mask
        return lax.dot_general(
            left[: 16 * groups, :],
            oh_lo[...],
            (((1,), (1,)), ((), ())),
            preferred_element_type=F32,
        )

    def cut(index, value):
        first = value.astype(BF16).astype(F32)
        pieces[2 * index] = first
        pieces[2 * index + 1] = value - first

    def joined(result, index):
        return result[32 * index : 32 * index + 16] + result[32 * index + 16 : 32 * index + 32]

    def project(vector):
        weights = wts[...]
        for row in range(2):
            running = cj_ref[9 * row].astype(F32) * wide(vector[0])
            for k in range(1, 9):
                running = running + cj_ref[9 * row + k].astype(F32) * wide(vector[k])
            err[row] = running * weights
        return err[0], err[1]

    def products(base, errors):
        for column_index in range(3):
            cut(
                base + column_index,
                errors[0] * pj_ref[column_index].astype(F32)
                + errors[1] * pj_ref[3 + column_index].astype(F32),
            )

    rows = [back_ref[:, 128 * t : 128 * (t + 1)] for t in range(3)]
    rows += [front_ref[:, 128 * t : 128 * (t + 1)] for t in range(3)]
    rows += [jnp.zeros((2, 128), jnp.int32)]
    listed = jnp.concatenate(rows, axis=0)
    list_lo, list_hi = listed & 127, listed >> 7
    flat = jnp.concatenate([back_ref[...], front_ref[...]], axis=1)
    width = flat.shape[1]
    flat_lo = spread((flat & 127).astype(F32), 128)
    flat_hi = spread((flat >> 7).astype(F32), 8)
    order = lax.broadcasted_iota(jnp.int32, (8, width), 1)
    hot_lo = jnp.where(
        flat_lo == lax.broadcasted_iota(jnp.int32, (128, width), 0).astype(F32), 1.0, 0.0
    ).astype(BF16)
    same_hi = flat_hi == lax.broadcasted_iota(jnp.int32, (8, width), 0).astype(F32)
    marks = jnp.concatenate(
        [
            jnp.where(same_hi, (order & 127).astype(F32), 0.0),
            jnp.where(same_hi, ((order >> 7) + 1).astype(F32), 0.0),
        ],
        axis=0,
    ).astype(BF16)
    places = lax.dot_general(
        marks, hot_lo, (((1,), (1,)), ((), ())), preferred_element_type=F32
    ).astype(jnp.int32)
    place_lo, place_hi = places[:8], places[8:16] - 1

    sub8 = lax.broadcasted_iota(jnp.int32, (8, 128), 0)
    back_rows = sub8 < 3

    def outgoing(sums, index, to_next, to_prev):
        own, outer = sums[:8], sums[8:16]
        picked = jnp.zeros((8, 128), F32)
        for h in range(8):
            found = lane_pick(spread(own[h : h + 1], 8), list_lo)
            picked = jnp.where(list_hi == h, found, picked)
        to_next[index] = jnp.where(back_rows, picked, outer)
        to_prev[index] = jnp.where(back_rows, outer, picked)

    def complete(sums, prev_block, next_block):
        own, outer = sums[:8], sums[8:16]
        mixed = jnp.where(back_rows, next_block, prev_block)
        added = jnp.zeros((8, 128), F32)
        for h in range(6):
            found = lane_pick(spread(mixed[h : h + 1], 8), place_lo)
            added = jnp.where(place_hi == h, found, added)
        return jnp.concatenate(
            [own + added, outer + jnp.where(back_rows, prev_block, next_block)], axis=0
        )

    obs_lo, obs_hi = stack(obs_ref[...] & 127), stack(obs_ref[...] >> 7)

    def solve(sums, inverse):
        return [
            inverse[0] * sums[0] + inverse[1] * sums[1] + inverse[2] * sums[2],
            inverse[1] * sums[0] + inverse[3] * sums[1] + inverse[4] * sums[2],
            inverse[2] * sums[0] + inverse[4] * sums[1] + inverse[5] * sums[2],
        ]

    def finish(vector, errors, points):
        for j in range(3):
            table[j] = points[j]
        picked = []
        for j in range(3):
            found = jnp.zeros((cams * tiles, 128), F32)
            for h in range(14):
                row = spread(table[j, h : h + 1, :], cams * tiles)
                found = jnp.where(obs_hi == h, lane_pick(row, obs_lo), found)
            picked.append(
                jnp.concatenate(
                    [found[cams * t : cams * (t + 1)] for t in range(tiles)], axis=1
                )
            )
        weights = wts[...]
        adjusted = []
        for row in range(2):
            term = picked[0] * pj_ref[3 * row].astype(F32)
            term = term + picked[1] * pj_ref[3 * row + 1].astype(F32)
            term = term + picked[2] * pj_ref[3 * row + 2].astype(F32)
            adjusted.append(errors[row] - weights * term)
        image = []
        for k in range(9):
            both = (
                cj_ref[k].astype(F32) * adjusted[0] + cj_ref[9 + k].astype(F32) * adjusted[1]
            )
            image.append(cam_damp * vector[k] + narrow_sum(both))
        return image

    for load in loads[5:]:
        load.wait()
    cam_damp = stand(cdamp_ref[...])
    right = [stand(rhs_ref[k : k + 1, :]) for k in range(9)]

    errors = project(guess)
    weights = wts[...]
    for i, (a, b) in enumerate(PAIRS):
        product = pj_ref[a].astype(F32) * pj_ref[b].astype(F32)
        product = product + pj_ref[3 + a].astype(F32) * pj_ref[3 + b].astype(F32)
        cut(i, product * weights)
    products(6, errors)
    result = scatter(18)
    sums = []
    damping = jnp.concatenate([damp_ref[...], jnp.zeros((8, 128), F32)], axis=0)
    for i in range(9):
        value = joined(result, i)
        if i < 6 and PAIRS[i][0] == PAIRS[i][1]:
            value = value + damping
        outgoing(value, i, next_out0, prev_out0)
        sums.append(value)
    pl.semaphore_wait(
        barrier,
        plane_size
        - hub.astype(jnp.int32)
        + hub.astype(jnp.int32) * (nz * nc - 1)
        + has_next.astype(jnp.int32)
        + has_prev.astype(jnp.int32),
    )
    copies = border_copies(0, next_out0, prev_out0, from_prev0, from_next0)
    border_start(copies)
    precond = []
    for k in range(9):
        square = cj_ref[k].astype(F32) ** 2 + cj_ref[9 + k].astype(F32) ** 2
        precond.append(recip(cam_damp + narrow_sum(square * weights)))
    border_wait(copies)
    sums = [complete(sums[i], from_prev0[i], from_next0[i]) for i in range(9)]
    ent = sums[:6]
    cofactors = [
        ent[3] * ent[5] - ent[4] * ent[4],
        ent[2] * ent[4] - ent[1] * ent[5],
        ent[1] * ent[4] - ent[2] * ent[3],
        ent[0] * ent[5] - ent[2] * ent[2],
        ent[1] * ent[2] - ent[0] * ent[4],
        ent[0] * ent[3] - ent[1] * ent[1],
    ]
    determinant = ent[0] * cofactors[0] + ent[1] * cofactors[1] + ent[2] * cofactors[2]
    scale = recip(jnp.where(determinant > 0.0, determinant, 1.0))
    inverse = [member * scale for member in cofactors]
    image = finish(guess, errors, solve(sums[6:], inverse))
    res0 = [right[k] - image[k] for k in range(9)]
    dir0 = [precond[k] * res0[k] for k in range(9)]

    def forward(vector, index):
        errors = project(vector)
        products(0, errors)
        result = scatter(6)
        sums = [joined(result, i) for i in range(3)]
        to_next, to_prev = next_out.at[index], prev_out.at[index]
        for i in range(3):
            outgoing(sums[i], i, to_next, to_prev)
        copies = border_copies(
            1 + index, to_next, to_prev, from_prev.at[index], from_next.at[index]
        )
        border_start(copies)
        return errors, sums, copies

    def arrived(index, sums):
        return [complete(sums[i], from_prev[index, i], from_next[index, i]) for i in range(3)]

    lane = lax.broadcasted_iota(jnp.int32, (1, 128), 1)

    errors, sums, copies = forward(dir0, 0)
    border_wait(copies)
    sums = arrived(0, sums)
    img0 = finish(dir0, errors, solve(sums, inverse))
    res_t = [res0[k] - img0[k] for k in range(9)]
    dir_t = [precond[k] * res_t[k] for k in range(9)]
    errors, sums, copies = forward(dir_t, 1)
    scalars = [
        inner(res0, dir0),
        inner(dir0, img0),
        inner(res_t, dir0),
        inner(img0, dir_t),
        inner(res_t, dir_t),
    ]
    row = jnp.zeros((1, 128), F32)
    for i, scalar in enumerate(scalars):
        row = jnp.where(lane == i, scalar, row)
    damped = jnp.sum(cam_damp * sum(entry * entry for entry in dir_t), axis=0, keepdims=True)
    squares = errors[0] * errors[0] + errors[1] * errors[1]
    squares = jnp.sum(squares, axis=0, keepdims=True)
    squares = sum(squares[:, 128 * t : 128 * (t + 1)] for t in range(tiles))
    border_wait(copies)
    sums = arrived(1, sums)
    points = solve(sums, inverse)
    energy = sum(sums[j][:8] * points[j][:8] for j in range(3))
    squares = squares - jnp.sum(energy, axis=0, keepdims=True)
    curve_t = damped + jnp.sum(squares, axis=1, keepdims=True)
    reduce_start(jnp.where(lane == len(scalars), curve_t, row))
    img_t = finish(dir_t, errors, points)
    row = reduce_finish()

    def at(index):
        picked = jnp.sum(jnp.where(lane == index, row, 0.0), axis=1, keepdims=True)
        return jnp.broadcast_to(picked, (1, 128))

    inner0, curve0, mixed_t, cross_t, inner_t, curve_t = [at(i) for i in range(6)]
    shift = mixed_t * recip(curve0)
    step0 = 1.0 + shift
    inner1 = inner_t - 2.0 * shift * cross_t + shift * shift * (curve0 - cross_t)
    curve1 = step0 * step0 * curve_t - 2.0 * shift * step0 * cross_t + shift * shift * curve0
    ratio = inner1 * recip(inner0)
    step1 = inner1 * recip(curve1 - ratio * inner1 * recip(step0))
    dir1 = [step0 * dir_t[k] - shift * dir0[k] for k in range(9)]
    res1 = [res_t[k] - shift * img0[k] for k in range(9)]
    img1 = [step0 * img_t[k] - shift * img0[k] for k in range(9)]
    for k in range(9):
        moved = guess[k] + step0 * dir0[k] + step1 * (dir1[k] + ratio * dir0[k])
        out_ref[0, k : k + 1, :] = lie(moved)
        left_over = res1[k] - step1 * (img1[k] + ratio * img0[k])
        out_ref[1, k : k + 1, :] = lie(left_over)


def local(dims, cam_jac, point_jac, obs_point, obs_count, back_list, front_list, point_damp,
          cam_damp, right_side, start_guess):
    cams, slots = obs_point.shape
    entries = cams * slots
    nx, nz, ny, nc = dims
    arrays = (
        cam_jac,
        point_jac,
        obs_point,
        obs_count.reshape(1, cams),
        back_list,
        front_list,
        point_damp.reshape(8, 128),
        cam_damp.reshape(1, cams),
        right_side,
        start_guess,
    )
    arrays = tuple(pltpu.with_memory_space_constraint(array, pltpu.HBM) for array in arrays)
    vmem = pl.BlockSpec(memory_space=pltpu.VMEM)
    shape = jax.ShapeDtypeStruct((2, *right_side.shape), F32)
    both = pl.pallas_call(
        functools.partial(kernel, dims),
        out_shape=shape,
        in_specs=[pl.BlockSpec(memory_space=pltpu.HBM)] * len(arrays),
        out_specs=vmem,
        scratch_shapes=[
            *[pltpu.VMEM(array.shape, array.dtype) for array in arrays],
            pltpu.SemaphoreType.DMA((len(arrays),)),
            pltpu.VMEM((128, entries), BF16),
            pltpu.VMEM((16, entries), BF16),
            pltpu.VMEM((288, entries), BF16),
            pltpu.VMEM((18, cams, slots), F32),
            pltpu.VMEM((2, cams, slots), F32),
            pltpu.VMEM((cams, slots), F32),
            pltpu.VMEM((3, 16, 128), F32),
            pltpu.VMEM((9, 8, 128), F32),
            pltpu.VMEM((9, 8, 128), F32),
            pltpu.VMEM((9, 8, 128), F32),
            pltpu.VMEM((9, 8, 128), F32),
            pltpu.VMEM((2, 3, 8, 128), F32),
            pltpu.VMEM((2, 3, 8, 128), F32),
            pltpu.VMEM((2, 3, 8, 128), F32),
            pltpu.VMEM((2, 3, 8, 128), F32),
            pltpu.VMEM((1, 128), F32),
            pltpu.VMEM((nx * ny * nc, 1, 128), F32),
            pltpu.VMEM((1, 128), F32),
            pltpu.VMEM((nz, 1, 128), F32),
            pltpu.SemaphoreType.DMA((3, 2)),
            pltpu.SemaphoreType.DMA((3, 2)),
            pltpu.SemaphoreType.DMA((nx * ny,)),
            pltpu.SemaphoreType.DMA((nx * ny * nc,)),
            pltpu.SemaphoreType.DMA((nz * nc,)),
            pltpu.SemaphoreType.DMA((nz,)),
        ],
        compiler_params=pltpu.CompilerParams(
            collective_id=0, has_side_effects=True, vmem_limit_bytes=48 * 1024 * 1024
        ),
    )(*arrays)
    return both[0], both[1]


def solution(mesh):
    seg = "seg"
    return jax.shard_map(
        functools.partial(local, DIMS),
        mesh=mesh,
        in_specs=(
            P(None, seg, None),
            P(None, seg, None),
            P(seg, None),
            P(seg),
            P(seg, None),
            P(seg, None),
            P(seg),
            P(seg),
            P(None, seg),
            P(None, seg),
        ),
        out_specs=(P(None, seg), P(None, seg)),
        check_vma=False,
    )
```

```python
import functools

import jax
import jax.numpy as jnp
from jax import lax
from jax.experimental import pallas as pl
from jax.experimental.pallas import tpu as pltpu
from jax.sharding import PartitionSpec as P

DIMS = (4, 8, 4, 2)
HUB = 1
PAIRS = ((0, 0), (0, 1), (0, 2), (1, 1), (1, 2), (2, 2))
F32 = jnp.float32
BF16 = jnp.bfloat16
F8 = jnp.float8_e4m3fn
MESH = pl.DeviceIdType.MESH


def spread(block, rows):
    return jnp.broadcast_to(block, (rows, block.shape[1]))


def lane_pick(row, index):
    return jnp.take_along_axis(row, index, axis=1, mode="promise_in_bounds")


def recip(value):
    first = 1.0 / value
    return first * (2.0 - value * first)


def kernel(
    dims,
    cj_hbm,
    pj_hbm,
    obs_hbm,
    cnt_hbm,
    back_hbm,
    front_hbm,
    damp_hbm,
    cdamp_hbm,
    rhs_hbm,
    guess_hbm,
    out_ref,
    cj_ref,
    pj_ref,
    obs_ref,
    cnt_ref,
    back_ref,
    front_ref,
    damp_ref,
    cdamp_ref,
    rhs_ref,
    guess_ref,
    load_sem,
    oh_lo,
    oh_hi,
    pieces,
    err,
    wts,
    table,
    rows_ref,
    next_out0,
    prev_out0,
    from_prev0,
    from_next0,
    next_out,
    prev_out,
    from_prev,
    from_next,
    first_out,
    first_in,
    second_out,
    second_in,
    ex_send,
    ex_recv,
    first_send,
    first_recv,
    second_send,
    second_recv,
):
    nx, nz, ny, nc = dims
    total = nx * nz * ny * nc
    arrivals = [
        (obs_hbm, obs_ref),
        (cnt_hbm, cnt_ref),
        (guess_hbm, guess_ref),
        (back_hbm, back_ref),
        (front_hbm, front_ref),
        (pj_hbm, pj_ref),
        (cj_hbm, cj_ref),
        (damp_hbm, damp_ref),
        (cdamp_hbm, cdamp_ref),
        (rhs_hbm, rhs_ref),
    ]
    loads = [
        pltpu.make_async_copy(source, target, load_sem.at[i])
        for i, (source, target) in enumerate(arrivals)
    ]
    for load in loads:
        load.start()
    cams, slots = obs_ref.shape
    tiles = slots // 128
    me = lax.axis_index("seg")
    core = lax.rem(me, nc)
    y = lax.rem(me // nc, ny)
    z = lax.rem(me // (nc * ny), nz)
    x = me // (nc * ny * nz)

    def ident(px, pz, py, pc):
        return ((px * nz + pz) * ny + py) * nc + pc

    plane_size = nx * ny
    hub = core == HUB

    def plane_at(step, sign):
        px = lax.rem(x + (step // ny if sign > 0 else nx - step // ny), nx)
        py = lax.rem(y + (step % ny if sign > 0 else ny - step % ny), ny)
        return px, py

    def height_at(step, sign):
        return lax.rem(z + (step if sign > 0 else nz - step), nz)

    has_next, has_prev = me < total - 1, me > 0

    barrier = pltpu.get_barrier_semaphore()

    def greet(device):
        pl.semaphore_signal(barrier, inc=1, device_id=(device,), device_id_type=MESH)

    @pl.when(hub)
    def _():
        for step in range(plane_size):
            px, py = plane_at(step, -1)
            for pc in range(nc):
                if step or pc != HUB:
                    greet(ident(px, z, py, pc))

    for step in range(1, nz):
        greet(ident(x, height_at(step, -1), y, HUB))

    @pl.when(jnp.logical_not(hub))
    def _():
        greet(ident(x, z, y, HUB))

    @pl.when(has_next)
    def _():
        pl.semaphore_signal(barrier, inc=1, device_id=(me + 1,), device_id_type=MESH)

    @pl.when(has_prev)
    def _():
        pl.semaphore_signal(barrier, inc=1, device_id=(me - 1,), device_id_type=MESH)

    @pl.when(jnp.logical_not(has_prev))
    def _():
        from_prev0[...] = jnp.zeros_like(from_prev0)
        from_prev[...] = jnp.zeros_like(from_prev)

    @pl.when(jnp.logical_not(has_next))
    def _():
        from_next0[...] = jnp.zeros_like(from_next0)
        from_next[...] = jnp.zeros_like(from_next)

    def border_copies(index, to_next, to_prev, came_prev, came_next):
        ahead = pltpu.make_async_remote_copy(
            src_ref=to_next,
            dst_ref=came_prev,
            send_sem=ex_send.at[index, 0],
            recv_sem=ex_recv.at[index, 0],
            device_id=(jnp.minimum(me + 1, total - 1),),
            device_id_type=MESH,
        )
        behind = pltpu.make_async_remote_copy(
            src_ref=to_prev,
            dst_ref=came_next,
            send_sem=ex_send.at[index, 1],
            recv_sem=ex_recv.at[index, 1],
            device_id=(jnp.maximum(me - 1, 0),),
            device_id_type=MESH,
        )
        return ahead, behind

    def border_start(copies):
        ahead, behind = copies

        @pl.when(has_next)
        def _():
            ahead.start()

        @pl.when(has_prev)
        def _():
            behind.start()

    def border_wait(copies):
        ahead, behind = copies

        @pl.when(has_prev)
        def _():
            ahead.wait_recv()
            behind.wait_send()

        @pl.when(has_next)
        def _():
            behind.wait_recv()
            ahead.wait_send()

    plane_me = (x * ny + y) * nc + core

    def first_copy(step, sender_core, slot):
        px, py = plane_at(step, 1)
        return pltpu.make_async_remote_copy(
            src_ref=first_out,
            dst_ref=first_in.at[slot],
            send_sem=first_send.at[step],
            recv_sem=first_recv.at[step * nc + sender_core],
            device_id=(ident(px, z, py, HUB),),
            device_id_type=MESH,
        )

    def second_copy(step, pc, slot):
        return pltpu.make_async_remote_copy(
            src_ref=second_out,
            dst_ref=second_in.at[slot],
            send_sem=second_send.at[step * nc + pc],
            recv_sem=second_recv.at[step],
            device_id=(ident(x, height_at(step, 1), y, pc),),
            device_id_type=MESH,
        )

    far_first = sorted(
        range(1, plane_size),
        key=lambda step: -(
            min(step // ny, nx - step // ny) + min(step % ny, ny - step % ny)
        ),
    )
    high_first = sorted(range(1, nz), key=lambda step: -min(step, nz - step))

    def tree(terms):
        while len(terms) > 1:
            terms = [sum(terms[i : i + 2]) for i in range(0, len(terms), 2)]
        return terms[0]

    def reduce_start(value):
        first_out[...] = value
        for step in far_first:
            first_copy(step, core, plane_me).start()

        @pl.when(hub)
        def _():
            first_in[plane_me] = value

        @pl.when(jnp.logical_not(hub))
        def _():
            first_copy(0, core, plane_me).start()

    def reduce_finish():
        @pl.when(hub)
        def _():
            for step in range(plane_size):
                px, py = plane_at(step, -1)
                for pc in range(nc):
                    if step or pc != HUB:
                        first_copy(step, pc, (px * ny + py) * nc + pc).wait_recv()
            value = tree([first_in[slot] for slot in range(plane_size * nc)])
            second_out[...] = value
            second_in[z] = value
            for step in high_first:
                for pc in range(nc):
                    second_copy(step, pc, z).start()
            for pc in range(nc):
                if pc != HUB:
                    second_copy(0, pc, z).start()

        for step in far_first:
            first_copy(step, core, plane_me).wait_send()

        @pl.when(jnp.logical_not(hub))
        def _():
            first_copy(0, core, plane_me).wait_send()
            second_copy(0, core, z).wait_recv()

        for step in range(1, nz):
            second_copy(step, core, height_at(step, -1)).wait_recv()

        @pl.when(hub)
        def _():
            for step in high_first:
                for pc in range(nc):
                    second_copy(step, pc, z).wait_send()
            for pc in range(nc):
                if pc != HUB:
                    second_copy(0, pc, z).wait_send()

        return tree([second_in[slot] for slot in range(nz)])

    eye = lax.broadcasted_iota(jnp.int32, (cams, cams), 0) == lax.broadcasted_iota(
        jnp.int32, (cams, cams), 1
    )

    def stand(row):
        summed = jnp.sum(jnp.where(eye, spread(row, cams), 0.0), axis=1, keepdims=True)
        return jnp.broadcast_to(summed, (cams, 128))

    eye_wide = lax.broadcasted_iota(jnp.int32, (cams, 128), 0) == lax.broadcasted_iota(
        jnp.int32, (cams, 128), 1
    )

    def lie(block):
        return jnp.sum(jnp.where(eye_wide, block, 0.0), axis=0, keepdims=True)[:, :cams]

    def wide(block):
        return jnp.concatenate([block] * tiles, axis=1)

    def stack(block):
        return jnp.concatenate(
            [block[:, 128 * t : 128 * (t + 1)] for t in range(tiles)], axis=0
        )

    def narrow_sum(block):
        summed = jnp.sum(block, axis=1, keepdims=True)
        return jnp.broadcast_to(summed, (cams, 128))

    def inner(first, second):
        running = first[0] * second[0]
        for k in range(1, 9):
            running = running + first[k] * second[k]
        return jnp.sum(running, axis=0, keepdims=True)

    for load in loads:
        load.wait()
    count = stand(cnt_ref[...].astype(F32))
    guess = [stand(guess_ref[k : k + 1, :]) for k in range(9)]
    position = lax.broadcasted_iota(jnp.int32, (cams, slots), 1).astype(F32)
    wts[...] = jnp.where(position < wide(count), 1.0, 0.0)

    lo_line = lax.broadcasted_iota(jnp.int32, (256, slots), 0).astype(F32).astype(BF16)
    hi_line = lax.broadcasted_iota(jnp.int32, (16, slots), 0)
    hi_line = (hi_line & 7).astype(F32).astype(BF16)
    one, none = jnp.ones((), BF16), jnp.zeros((), BF16)
    for c in range(cams):
        row = obs_ref[c : c + 1, :]
        low = ((row & 127) + ((row >> 10) << 7)).astype(F32)
        high = ((row >> 7) & 7).astype(F32)
        here = pl.ds(c * slots, slots)
        hit = jnp.where(spread(low, 256).astype(BF16) == lo_line, one, none)
        oh_lo[:, here] = hit.astype(F8)
        oh_hi[:, here] = jnp.where(spread(high, 16).astype(BF16) == hi_line, one, none)

    def scatter(values):
        total = None
        for c in range(cams):
            here = pl.ds(c * slots, slots)
            mask = oh_hi[:, here]
            rows = []
            for v in range(values):
                pair = [spread(pieces[2 * v + p, c : c + 1, :], 8) for p in range(2)]
                rows.append(jnp.concatenate(pair, axis=0).astype(BF16) * mask)
            part = lax.dot_general(
                jnp.concatenate(rows, axis=0),
                oh_lo[:, here],
                (((1,), (1,)), ((), ())),
                preferred_element_type=F32,
            )
            total = part if total is None else total + part
        return total

    def cut(index, value):
        first = value.astype(BF16).astype(F32)
        pieces[2 * index] = first
        pieces[2 * index + 1] = value - first

    def joined(result, index):
        both = result[16 * index : 16 * index + 8] + result[16 * index + 8 : 16 * index + 16]
        return jnp.concatenate([both[:, :128], both[:, 128:]], axis=0)

    def project(vector):
        weights = wts[...]
        for row in range(2):
            running = cj_ref[9 * row].astype(F32) * wide(vector[0])
            for k in range(1, 9):
                running = running + cj_ref[9 * row + k].astype(F32) * wide(vector[k])
            err[row] = running * weights
        return err[0], err[1]

    def products(base, errors):
        for column_index in range(3):
            cut(
                base + column_index,
                errors[0] * pj_ref[column_index].astype(F32)
                + errors[1] * pj_ref[3 + column_index].astype(F32),
            )

    rows = [back_ref[:, 128 * t : 128 * (t + 1)] for t in range(3)]
    rows += [front_ref[:, 128 * t : 128 * (t + 1)] for t in range(3)]
    rows += [jnp.zeros((2, 128), jnp.int32)]
    listed = jnp.concatenate(rows, axis=0)
    list_lo, list_hi = listed & 127, listed >> 7
    flat = jnp.concatenate([back_ref[...], front_ref[...]], axis=1)
    width = flat.shape[1]
    flat_lo = spread((flat & 127).astype(F32), 128)
    flat_hi = spread((flat >> 7).astype(F32), 8)
    order = lax.broadcasted_iota(jnp.int32, (8, width), 1)
    hot_lo = jnp.where(
        flat_lo == lax.broadcasted_iota(jnp.int32, (128, width), 0).astype(F32), 1.0, 0.0
    ).astype(BF16)
    same_hi = flat_hi == lax.broadcasted_iota(jnp.int32, (8, width), 0).astype(F32)
    marks = jnp.concatenate(
        [
            jnp.where(same_hi, (order & 127).astype(F32), 0.0),
            jnp.where(same_hi, ((order >> 7) + 1).astype(F32), 0.0),
        ],
        axis=0,
    ).astype(BF16)
    places = lax.dot_general(
        marks, hot_lo, (((1,), (1,)), ((), ())), preferred_element_type=F32
    ).astype(jnp.int32)
    place_lo, place_hi = places[:8], places[8:16] - 1

    sub8 = lax.broadcasted_iota(jnp.int32, (8, 128), 0)
    back_rows = sub8 < 3

    def outgoing(sums, index, to_next, to_prev):
        own, outer = sums[:8], sums[8:16]
        picked = jnp.zeros((8, 128), F32)
        for h in range(8):
            found = lane_pick(spread(own[h : h + 1], 8), list_lo)
            picked = jnp.where(list_hi == h, found, picked)
        to_next[index] = jnp.where(back_rows, picked, outer)
        to_prev[index] = jnp.where(back_rows, outer, picked)

    def complete(sums, prev_block, next_block):
        own, outer = sums[:8], sums[8:16]
        mixed = jnp.where(back_rows, next_block, prev_block)
        added = jnp.zeros((8, 128), F32)
        for h in range(6):
            found = lane_pick(spread(mixed[h : h + 1], 8), place_lo)
            added = jnp.where(place_hi == h, found, added)
        return jnp.concatenate(
            [own + added, outer + jnp.where(back_rows, prev_block, next_block)], axis=0
        )

    obs_lo, obs_hi = stack(obs_ref[...] & 127), stack(obs_ref[...] >> 7)

    def solve(sums, inverse):
        return [
            inverse[0] * sums[0] + inverse[1] * sums[1] + inverse[2] * sums[2],
            inverse[1] * sums[0] + inverse[3] * sums[1] + inverse[4] * sums[2],
            inverse[2] * sums[0] + inverse[4] * sums[1] + inverse[5] * sums[2],
        ]

    def finish(vector, errors, points):
        for j in range(3):
            table[j] = points[j]
        found = [[] for _ in range(3)]
        for block in range(cams * tiles // 8):
            low, high = (part[8 * block : 8 * block + 8] for part in (obs_lo, obs_hi))
            masks = [high == h for h in range(14)]
            for j in range(3):
                value = jnp.zeros((8, 128), F32)
                for h in range(14):
                    row = spread(table[j, h : h + 1, :], 8)
                    value = jnp.where(masks[h], lane_pick(row, low), value)
                found[j].append(value)
        picked = [
            jnp.concatenate(
                [
                    jnp.concatenate(found[j][cams // 8 * t : cams // 8 * (t + 1)], axis=0)
                    for t in range(tiles)
                ],
                axis=1,
            )
            for j in range(3)
        ]
        weights = wts[...]
        adjusted = []
        for row in range(2):
            term = picked[0] * pj_ref[3 * row].astype(F32)
            term = term + picked[1] * pj_ref[3 * row + 1].astype(F32)
            term = term + picked[2] * pj_ref[3 * row + 2].astype(F32)
            adjusted.append(errors[row] - weights * term)
        image = []
        for k in range(9):
            both = (
                cj_ref[k].astype(F32) * adjusted[0] + cj_ref[9 + k].astype(F32) * adjusted[1]
            )
            image.append(cam_damp * vector[k] + narrow_sum(both))
        return image

    cam_damp = stand(cdamp_ref[...])
    right = [stand(rhs_ref[k : k + 1, :]) for k in range(9)]

    errors = project(guess)
    weights = wts[...]
    for i, (a, b) in enumerate(PAIRS):
        product = pj_ref[a].astype(F32) * pj_ref[b].astype(F32)
        product = product + pj_ref[3 + a].astype(F32) * pj_ref[3 + b].astype(F32)
        cut(i, product * weights)
    products(6, errors)
    result = scatter(9)
    sums = []
    damping = jnp.concatenate([damp_ref[...], jnp.zeros((8, 128), F32)], axis=0)
    for i in range(9):
        value = joined(result, i)
        if i < 6 and PAIRS[i][0] == PAIRS[i][1]:
            value = value + damping
        outgoing(value, i, next_out0, prev_out0)
        sums.append(value)
    pl.semaphore_wait(
        barrier,
        plane_size
        - hub.astype(jnp.int32)
        + hub.astype(jnp.int32) * (nz * nc - 1)
        + has_next.astype(jnp.int32)
        + has_prev.astype(jnp.int32),
    )
    copies = border_copies(0, next_out0, prev_out0, from_prev0, from_next0)
    border_start(copies)
    precond = []
    for k in range(9):
        square = cj_ref[k].astype(F32) ** 2 + cj_ref[9 + k].astype(F32) ** 2
        precond.append(recip(cam_damp + narrow_sum(square * weights)))
    border_wait(copies)
    sums = [complete(sums[i], from_prev0[i], from_next0[i]) for i in range(9)]
    ent = sums[:6]
    cofactors = [
        ent[3] * ent[5] - ent[4] * ent[4],
        ent[2] * ent[4] - ent[1] * ent[5],
        ent[1] * ent[4] - ent[2] * ent[3],
        ent[0] * ent[5] - ent[2] * ent[2],
        ent[1] * ent[2] - ent[0] * ent[4],
        ent[0] * ent[3] - ent[1] * ent[1],
    ]
    determinant = ent[0] * cofactors[0] + ent[1] * cofactors[1] + ent[2] * cofactors[2]
    scale = recip(jnp.where(determinant > 0.0, determinant, 1.0))
    inverse = [member * scale for member in cofactors]
    image = finish(guess, errors, solve(sums[6:], inverse))
    res0 = [right[k] - image[k] for k in range(9)]
    dir0 = [precond[k] * res0[k] for k in range(9)]

    def forward(vector, index):
        errors = project(vector)
        products(0, errors)
        result = scatter(3)
        sums = [joined(result, i) for i in range(3)]
        to_next, to_prev = next_out.at[index], prev_out.at[index]
        for i in range(3):
            outgoing(sums[i], i, to_next, to_prev)
        copies = border_copies(
            1 + index, to_next, to_prev, from_prev.at[index], from_next.at[index]
        )
        border_start(copies)
        return errors, sums, copies

    def arrived(index, sums):
        return [complete(sums[i], from_prev[index, i], from_next[index, i]) for i in range(3)]

    lane = lax.broadcasted_iota(jnp.int32, (1, 128), 1)

    errors, sums, copies = forward(dir0, 0)
    border_wait(copies)
    sums = arrived(0, sums)
    img0 = finish(dir0, errors, solve(sums, inverse))
    res_t = [res0[k] - img0[k] for k in range(9)]
    dir_t = [precond[k] * res_t[k] for k in range(9)]
    errors, sums, copies = forward(dir_t, 1)
    scalars = [
        inner(res0, dir0),
        inner(dir0, img0),
        inner(res_t, dir0),
        inner(img0, dir_t),
        inner(res_t, dir_t),
    ]
    row = jnp.zeros((1, 128), F32)
    for i, scalar in enumerate(scalars):
        row = jnp.where(lane == i, scalar, row)
    damped = jnp.sum(cam_damp * sum(entry * entry for entry in dir_t), axis=0, keepdims=True)
    squares = errors[0] * errors[0] + errors[1] * errors[1]
    squares = jnp.sum(squares, axis=0, keepdims=True)
    squares = sum(squares[:, 128 * t : 128 * (t + 1)] for t in range(tiles))
    border_wait(copies)
    sums = arrived(1, sums)
    points = solve(sums, inverse)
    energy = sum(sums[j][:8] * points[j][:8] for j in range(3))
    squares = squares - jnp.sum(energy, axis=0, keepdims=True)
    curve_t = damped + jnp.sum(squares, axis=1, keepdims=True)
    reduce_start(jnp.where(lane == len(scalars), curve_t, row))
    img_t = finish(dir_t, errors, points)
    flat_rows = [
        jnp.concatenate([lie(entry) for entry in vector], axis=0)
        for vector in (guess, dir0, dir_t, res_t, img0, img_t)
    ]
    for i, block in enumerate(flat_rows):
        rows_ref[i] = block
    row = reduce_finish()

    def at(index):
        picked = jnp.sum(jnp.where(lane == index, row, 0.0), axis=1, keepdims=True)
        return jnp.broadcast_to(picked, (1, 128))

    inner0, curve0, mixed_t, cross_t, inner_t, curve_t = [at(i) for i in range(6)]
    shift = mixed_t * recip(curve0)
    step0 = 1.0 + shift
    inner1 = inner_t - 2.0 * shift * cross_t + shift * shift * (curve0 - cross_t)
    curve1 = step0 * step0 * curve_t - 2.0 * shift * step0 * cross_t + shift * shift * curve0
    ratio = inner1 * recip(inner0)
    step1 = inner1 * recip(curve1 - ratio * inner1 * recip(step0))
    first_part = (step0 + step1 * (ratio - shift))[:, :cams]
    image_part = (shift + step1 * (ratio - shift))[:, :cams]
    second_part = (step1 * step0)[:, :cams]
    out_ref[0] = rows_ref[0] + first_part * rows_ref[1] + second_part * rows_ref[2]
    out_ref[1] = rows_ref[3] - image_part * rows_ref[4] - second_part * rows_ref[5]


def local(dims, cam_jac, point_jac, obs_point, obs_count, back_list, front_list, point_damp,
          cam_damp, right_side, start_guess):
    cams, slots = obs_point.shape
    entries = cams * slots
    nx, nz, ny, nc = dims
    arrays = (
        cam_jac,
        point_jac,
        obs_point,
        obs_count.reshape(1, cams),
        back_list,
        front_list,
        point_damp.reshape(8, 128),
        cam_damp.reshape(1, cams),
        right_side,
        start_guess,
    )
    arrays = tuple(pltpu.with_memory_space_constraint(array, pltpu.HBM) for array in arrays)
    vmem = pl.BlockSpec(memory_space=pltpu.VMEM)
    shape = jax.ShapeDtypeStruct((2, *right_side.shape), F32)
    both = pl.pallas_call(
        functools.partial(kernel, dims),
        out_shape=shape,
        in_specs=[pl.BlockSpec(memory_space=pltpu.HBM)] * len(arrays),
        out_specs=vmem,
        scratch_shapes=[
            *[pltpu.VMEM(array.shape, array.dtype) for array in arrays],
            pltpu.SemaphoreType.DMA((len(arrays),)),
            pltpu.VMEM((256, entries), F8),
            pltpu.VMEM((16, entries), BF16),
            pltpu.VMEM((18, cams, slots), F32),
            pltpu.VMEM((2, cams, slots), F32),
            pltpu.VMEM((cams, slots), F32),
            pltpu.VMEM((3, 16, 128), F32),
            pltpu.VMEM((6, 9, cams), F32),
            pltpu.VMEM((9, 8, 128), F32),
            pltpu.VMEM((9, 8, 128), F32),
            pltpu.VMEM((9, 8, 128), F32),
            pltpu.VMEM((9, 8, 128), F32),
            pltpu.VMEM((2, 3, 8, 128), F32),
            pltpu.VMEM((2, 3, 8, 128), F32),
            pltpu.VMEM((2, 3, 8, 128), F32),
            pltpu.VMEM((2, 3, 8, 128), F32),
            pltpu.VMEM((1, 128), F32),
            pltpu.VMEM((nx * ny * nc, 1, 128), F32),
            pltpu.VMEM((1, 128), F32),
            pltpu.VMEM((nz, 1, 128), F32),
            pltpu.SemaphoreType.DMA((3, 2)),
            pltpu.SemaphoreType.DMA((3, 2)),
            pltpu.SemaphoreType.DMA((nx * ny,)),
            pltpu.SemaphoreType.DMA((nx * ny * nc,)),
            pltpu.SemaphoreType.DMA((nz * nc,)),
            pltpu.SemaphoreType.DMA((nz,)),
        ],
        compiler_params=pltpu.CompilerParams(
            collective_id=0, has_side_effects=True, vmem_limit_bytes=48 * 1024 * 1024
        ),
    )(*arrays)
    return both[0], both[1]


def solution(mesh):
    seg = "seg"
    return jax.shard_map(
        functools.partial(local, DIMS),
        mesh=mesh,
        in_specs=(
            P(None, seg, None),
            P(None, seg, None),
            P(seg, None),
            P(seg),
            P(seg, None),
            P(seg, None),
            P(seg),
            P(seg),
            P(None, seg),
            P(None, seg),
        ),
        out_specs=(P(None, seg), P(None, seg)),
        check_vma=False,
    )
```

```python
import functools

import jax
import jax.numpy as jnp
from jax import lax
from jax.experimental import pallas as pl
from jax.experimental.pallas import tpu as pltpu
from jax.sharding import PartitionSpec as P

DIMS = (4, 8, 4, 2)
HUB = 1
PAIRS = ((0, 0), (0, 1), (0, 2), (1, 1), (1, 2), (2, 2))
F32 = jnp.float32
BF16 = jnp.bfloat16
F8 = jnp.float8_e4m3fn
MESH = pl.DeviceIdType.MESH


def spread(block, rows):
    return jnp.broadcast_to(block, (rows, block.shape[1]))


def lane_pick(row, index):
    return jnp.take_along_axis(row, index, axis=1, mode="promise_in_bounds")


def recip(value):
    first = 1.0 / value
    return first * (2.0 - value * first)


def kernel(
    dims,
    cj_hbm,
    pj_hbm,
    obs_hbm,
    cnt_hbm,
    back_hbm,
    front_hbm,
    damp_hbm,
    cdamp_hbm,
    rhs_hbm,
    guess_hbm,
    out_ref,
    cj_ref,
    pj_ref,
    obs_ref,
    cnt_ref,
    back_ref,
    front_ref,
    damp_ref,
    cdamp_ref,
    rhs_ref,
    guess_ref,
    load_sem,
    oh_lo,
    oh_hi,
    oh_lo2,
    oh_hi2,
    pieces,
    err,
    wts,
    table,
    rows_ref,
    next_out0,
    prev_out0,
    from_prev0,
    from_next0,
    next_out,
    prev_out,
    from_prev,
    from_next,
    first_out,
    first_in,
    second_out,
    second_in,
    ex_send,
    ex_recv,
    first_send,
    first_recv,
    second_send,
    second_recv,
):
    nx, nz, ny, nc = dims
    total = nx * nz * ny * nc
    arrivals = [
        (obs_hbm, obs_ref),
        (cnt_hbm, cnt_ref),
        (guess_hbm, guess_ref),
        (back_hbm, back_ref),
        (front_hbm, front_ref),
        (pj_hbm, pj_ref),
        *[(cj_hbm.at[pl.ds(6 * i, 6)], cj_ref.at[pl.ds(6 * i, 6)]) for i in range(3)],
        (damp_hbm, damp_ref),
        (cdamp_hbm, cdamp_ref),
        (rhs_hbm, rhs_ref),
    ]
    loads = [
        pltpu.make_async_copy(source, target, load_sem.at[i])
        for i, (source, target) in enumerate(arrivals)
    ]
    for load in loads:
        load.start()
    cams, slots = obs_ref.shape
    tiles = slots // 128
    me = lax.axis_index("seg")
    core = lax.rem(me, nc)
    y = lax.rem(me // nc, ny)
    z = lax.rem(me // (nc * ny), nz)
    x = me // (nc * ny * nz)

    def ident(px, pz, py, pc):
        return ((px * nz + pz) * ny + py) * nc + pc

    plane_size = nx * ny
    hub = core == HUB

    def plane_at(step, sign):
        px = lax.rem(x + (step // ny if sign > 0 else nx - step // ny), nx)
        py = lax.rem(y + (step % ny if sign > 0 else ny - step % ny), ny)
        return px, py

    def height_at(step, sign):
        return lax.rem(z + (step if sign > 0 else nz - step), nz)

    has_next, has_prev = me < total - 1, me > 0

    barrier = pltpu.get_barrier_semaphore()

    def greet(device):
        pl.semaphore_signal(barrier, inc=1, device_id=(device,), device_id_type=MESH)

    @pl.when(hub)
    def _():
        for step in range(plane_size):
            px, py = plane_at(step, -1)
            for pc in range(nc):
                if step or pc != HUB:
                    greet(ident(px, z, py, pc))

    for step in range(1, nz):
        greet(ident(x, height_at(step, -1), y, HUB))

    @pl.when(jnp.logical_not(hub))
    def _():
        greet(ident(x, z, y, HUB))

    @pl.when(has_next)
    def _():
        pl.semaphore_signal(barrier, inc=1, device_id=(me + 1,), device_id_type=MESH)

    @pl.when(has_prev)
    def _():
        pl.semaphore_signal(barrier, inc=1, device_id=(me - 1,), device_id_type=MESH)

    @pl.when(jnp.logical_not(has_prev))
    def _():
        from_prev0[...] = jnp.zeros_like(from_prev0)
        from_prev[...] = jnp.zeros_like(from_prev)

    @pl.when(jnp.logical_not(has_next))
    def _():
        from_next0[...] = jnp.zeros_like(from_next0)
        from_next[...] = jnp.zeros_like(from_next)

    def border_copies(index, to_next, to_prev, came_prev, came_next):
        ahead = pltpu.make_async_remote_copy(
            src_ref=to_next,
            dst_ref=came_prev,
            send_sem=ex_send.at[index, 0],
            recv_sem=ex_recv.at[index, 0],
            device_id=(jnp.minimum(me + 1, total - 1),),
            device_id_type=MESH,
        )
        behind = pltpu.make_async_remote_copy(
            src_ref=to_prev,
            dst_ref=came_next,
            send_sem=ex_send.at[index, 1],
            recv_sem=ex_recv.at[index, 1],
            device_id=(jnp.maximum(me - 1, 0),),
            device_id_type=MESH,
        )
        return ahead, behind

    def border_start(copies):
        ahead, behind = copies

        @pl.when(has_next)
        def _():
            ahead.start()

        @pl.when(has_prev)
        def _():
            behind.start()

    def border_wait(copies):
        ahead, behind = copies

        @pl.when(has_prev)
        def _():
            ahead.wait_recv()

        @pl.when(has_next)
        def _():
            behind.wait_recv()

    def border_sent(copies):
        ahead, behind = copies

        @pl.when(has_prev)
        def _():
            behind.wait_send()

        @pl.when(has_next)
        def _():
            ahead.wait_send()

    plane_me = (x * ny + y) * nc + core

    def first_copy(step, sender_core, slot):
        px, py = plane_at(step, 1)
        return pltpu.make_async_remote_copy(
            src_ref=first_out,
            dst_ref=first_in.at[slot],
            send_sem=first_send.at[step],
            recv_sem=first_recv.at[step * nc + sender_core],
            device_id=(ident(px, z, py, HUB),),
            device_id_type=MESH,
        )

    def second_copy(step, pc, slot):
        return pltpu.make_async_remote_copy(
            src_ref=second_out,
            dst_ref=second_in.at[slot],
            send_sem=second_send.at[step * nc + pc],
            recv_sem=second_recv.at[step],
            device_id=(ident(x, height_at(step, 1), y, pc),),
            device_id_type=MESH,
        )

    far_first = sorted(
        range(1, plane_size),
        key=lambda step: -(
            min(step // ny, nx - step // ny) + min(step % ny, ny - step % ny)
        ),
    )
    high_first = sorted(range(1, nz), key=lambda step: -min(step, nz - step))

    def tree(terms):
        while len(terms) > 1:
            terms = [sum(terms[i : i + 2]) for i in range(0, len(terms), 2)]
        return terms[0]

    def reduce_start(value):
        first_out[...] = value
        for step in far_first:
            first_copy(step, core, plane_me).start()

        @pl.when(hub)
        def _():
            first_in[plane_me] = value

        @pl.when(jnp.logical_not(hub))
        def _():
            first_copy(0, core, plane_me).start()

    def reduce_finish():
        @pl.when(hub)
        def _():
            for step in range(plane_size):
                px, py = plane_at(step, -1)
                for pc in range(nc):
                    if step or pc != HUB:
                        first_copy(step, pc, (px * ny + py) * nc + pc).wait_recv()
            value = tree([first_in[slot] for slot in range(plane_size * nc)])
            second_out[...] = value
            second_in[z] = value
            for step in high_first:
                for pc in range(nc):
                    second_copy(step, pc, z).start()
            for pc in range(nc):
                if pc != HUB:
                    second_copy(0, pc, z).start()

        @pl.when(jnp.logical_not(hub))
        def _():
            second_copy(0, core, z).wait_recv()

        for step in range(1, nz):
            second_copy(step, core, height_at(step, -1)).wait_recv()

        return tree([second_in[slot] for slot in range(nz)])

    def reduce_sent():
        for step in far_first:
            first_copy(step, core, plane_me).wait_send()

        @pl.when(jnp.logical_not(hub))
        def _():
            first_copy(0, core, plane_me).wait_send()

        @pl.when(hub)
        def _():
            for step in high_first:
                for pc in range(nc):
                    second_copy(step, pc, z).wait_send()
            for pc in range(nc):
                if pc != HUB:
                    second_copy(0, pc, z).wait_send()

    eye = lax.broadcasted_iota(jnp.int32, (cams, cams), 0) == lax.broadcasted_iota(
        jnp.int32, (cams, cams), 1
    )

    def stand(row):
        summed = jnp.sum(jnp.where(eye, spread(row, cams), 0.0), axis=1, keepdims=True)
        return jnp.broadcast_to(summed, (cams, 128))

    eye_wide = lax.broadcasted_iota(jnp.int32, (cams, 128), 0) == lax.broadcasted_iota(
        jnp.int32, (cams, 128), 1
    )

    def lie(block):
        return jnp.sum(jnp.where(eye_wide, block, 0.0), axis=0, keepdims=True)[:, :cams]

    def wide(block):
        return jnp.concatenate([block] * tiles, axis=1)

    def stack(block):
        return jnp.concatenate(
            [block[:, 128 * t : 128 * (t + 1)] for t in range(tiles)], axis=0
        )

    def narrow_sum(block):
        summed = jnp.sum(block, axis=1, keepdims=True)
        return jnp.broadcast_to(summed, (cams, 128))

    def inner(first, second):
        running = first[0] * second[0]
        for k in range(1, 9):
            running = running + first[k] * second[k]
        return jnp.sum(running, axis=0, keepdims=True)

    for load in loads:
        load.wait()
    count = stand(cnt_ref[...].astype(F32))
    guess = [stand(guess_ref[k : k + 1, :]) for k in range(9)]
    position = lax.broadcasted_iota(jnp.int32, (cams, slots), 1).astype(F32)
    wts[...] = jnp.where(position < wide(count), 1.0, 0.0)

    lo_line = lax.broadcasted_iota(jnp.int32, (256, slots), 0).astype(F32).astype(BF16)
    hi_line = lax.broadcasted_iota(jnp.int32, (16, slots), 0)
    hi_line = (hi_line & 7).astype(F32).astype(BF16)
    one, none = jnp.ones((), BF16), jnp.zeros((), BF16)
    for c in range(cams):
        row = obs_ref[c : c + 1, :]
        low = ((row & 127) + ((row >> 10) << 7)).astype(F32)
        high = ((row >> 7) & 7).astype(F32)
        here = pl.ds(c * slots, slots)
        hit = jnp.where(spread(low, 256).astype(BF16) == lo_line, one, none)
        oh_lo[:, here] = hit.astype(F8)
        oh_hi[:, here] = jnp.where(spread(high, 16).astype(BF16) == hi_line, one if c % 2 == 0 else -one, none)

    def scatter(values):
        halves = [None, None]
        for c in range(cams):
            here = pl.ds(c * slots, slots)
            mask = oh_hi[:, here]
            rows = []
            for v in range(values):
                pair = [spread(pieces[2 * v + p, c : c + 1, :], 8) for p in range(2)]
                rows.append(jnp.concatenate(pair, axis=0).astype(BF16) * mask)
            part = lax.dot_general(
                jnp.concatenate(rows, axis=0),
                oh_lo[:, here],
                (((1,), (1,)), ((), ())),
                preferred_element_type=F32,
            )
            before = halves[c % 2]
            halves[c % 2] = part if before is None else before + part
        return halves[0] - halves[1]

    def scatter_wide(values):
        halves = [None, None]
        for c in range(cams):
            here = pl.ds(c * slots, slots)
            mask = oh_hi2[:, here]
            rows = [
                spread(pieces[g, c : c + 1, :], 16).astype(BF16) * mask
                for g in range(2 * values)
            ]
            part = lax.dot_general(
                jnp.concatenate(rows, axis=0),
                oh_lo2[:, here],
                (((1,), (1,)), ((), ())),
                preferred_element_type=F32,
            )
            before = halves[c % 2]
            halves[c % 2] = part if before is None else before + part
        return halves[0] - halves[1]

    def cut(index, value):
        first = value.astype(BF16).astype(F32)
        pieces[2 * index] = first
        pieces[2 * index + 1] = value - first

    def joined(result, index):
        both = result[16 * index : 16 * index + 8] + result[16 * index + 8 : 16 * index + 16]
        return jnp.concatenate([both[:, :128], both[:, 128:]], axis=0)

    def project(vector):
        weights = wts[...]
        for row in range(2):
            running = cj_ref[9 * row].astype(F32) * wide(vector[0])
            for k in range(1, 9):
                running = running + cj_ref[9 * row + k].astype(F32) * wide(vector[k])
            err[row] = running * weights
        return err[0], err[1]

    def products(base, errors):
        for column_index in range(3):
            cut(
                base + column_index,
                errors[0] * pj_ref[column_index].astype(F32)
                + errors[1] * pj_ref[3 + column_index].astype(F32),
            )

    rows = [back_ref[:, 128 * t : 128 * (t + 1)] for t in range(3)]
    rows += [front_ref[:, 128 * t : 128 * (t + 1)] for t in range(3)]
    rows += [jnp.zeros((2, 128), jnp.int32)]
    listed = jnp.concatenate(rows, axis=0)
    list_lo, list_hi = listed & 127, listed >> 7
    flat = jnp.concatenate([back_ref[...], front_ref[...]], axis=1)
    width = flat.shape[1]
    flat_lo = spread((flat & 127).astype(F32), 128)
    flat_hi = spread((flat >> 7).astype(F32), 8)
    order = lax.broadcasted_iota(jnp.int32, (8, width), 1)
    hot_lo = jnp.where(
        flat_lo == lax.broadcasted_iota(jnp.int32, (128, width), 0).astype(F32), 1.0, 0.0
    ).astype(BF16)
    same_hi = flat_hi == lax.broadcasted_iota(jnp.int32, (8, width), 0).astype(F32)
    marks = jnp.concatenate(
        [
            jnp.where(same_hi, (order & 127).astype(F32), 0.0),
            jnp.where(same_hi, ((order >> 7) + 1).astype(F32), 0.0),
        ],
        axis=0,
    ).astype(BF16)
    places = lax.dot_general(
        marks, hot_lo, (((1,), (1,)), ((), ())), preferred_element_type=F32
    ).astype(jnp.int32)
    place_lo, place_hi = places[:8], places[8:16] - 1

    sub8 = lax.broadcasted_iota(jnp.int32, (8, 128), 0)
    back_rows = sub8 < 3

    def outgoing(sums, index, to_next, to_prev):
        own, outer = sums[:8], sums[8:16]
        picked = jnp.zeros((8, 128), F32)
        for h in range(8):
            found = lane_pick(spread(own[h : h + 1], 8), list_lo)
            picked = jnp.where(list_hi == h, found, picked)
        to_next[index] = jnp.where(back_rows, picked, outer)
        to_prev[index] = jnp.where(back_rows, outer, picked)

    def complete(sums, prev_block, next_block):
        own, outer = sums[:8], sums[8:16]
        mixed = jnp.where(back_rows, next_block, prev_block)
        added = jnp.zeros((8, 128), F32)
        for h in range(6):
            found = lane_pick(spread(mixed[h : h + 1], 8), place_lo)
            added = jnp.where(place_hi == h, found, added)
        return jnp.concatenate(
            [own + added, outer + jnp.where(back_rows, prev_block, next_block)], axis=0
        )

    obs_lo, obs_hi = stack(obs_ref[...] & 127), stack(obs_ref[...] >> 7)

    def solve(sums, inverse):
        return [
            inverse[0] * sums[0] + inverse[1] * sums[1] + inverse[2] * sums[2],
            inverse[1] * sums[0] + inverse[3] * sums[1] + inverse[4] * sums[2],
            inverse[2] * sums[0] + inverse[4] * sums[1] + inverse[5] * sums[2],
        ]

    def finish(vector, errors, points):
        for j in range(3):
            table[j] = points[j]
        found = [[] for _ in range(3)]
        for block in range(cams * tiles // 8):
            low, high = (part[8 * block : 8 * block + 8] for part in (obs_lo, obs_hi))
            masks = [high == h for h in range(14)]
            for j in range(3):
                value = jnp.zeros((8, 128), F32)
                for h in range(14):
                    row = spread(table[j, h : h + 1, :], 8)
                    value = jnp.where(masks[h], lane_pick(row, low), value)
                found[j].append(value)
        picked = [
            jnp.concatenate(
                [
                    jnp.concatenate(found[j][cams // 8 * t : cams // 8 * (t + 1)], axis=0)
                    for t in range(tiles)
                ],
                axis=1,
            )
            for j in range(3)
        ]
        weights = wts[...]
        adjusted = []
        for row in range(2):
            term = picked[0] * pj_ref[3 * row].astype(F32)
            term = term + picked[1] * pj_ref[3 * row + 1].astype(F32)
            term = term + picked[2] * pj_ref[3 * row + 2].astype(F32)
            adjusted.append(errors[row] - weights * term)
        image = []
        for k in range(9):
            both = (
                cj_ref[k].astype(F32) * adjusted[0] + cj_ref[9 + k].astype(F32) * adjusted[1]
            )
            image.append(cam_damp * vector[k] + narrow_sum(both))
        return image

    cam_damp = stand(cdamp_ref[...])
    right = [stand(rhs_ref[k : k + 1, :]) for k in range(9)]

    errors = project(guess)
    weights = wts[...]
    for i, (a, b) in enumerate(PAIRS):
        product = pj_ref[a].astype(F32) * pj_ref[b].astype(F32)
        product = product + pj_ref[3 + a].astype(F32) * pj_ref[3 + b].astype(F32)
        cut(i, product * weights)
    products(6, errors)
    result = scatter(9)
    sums = []
    damping = jnp.concatenate([damp_ref[...], jnp.zeros((8, 128), F32)], axis=0)
    for i in range(9):
        value = joined(result, i)
        if i < 6 and PAIRS[i][0] == PAIRS[i][1]:
            value = value + damping
        outgoing(value, i, next_out0, prev_out0)
        sums.append(value)
    pl.semaphore_wait(
        barrier,
        plane_size
        - hub.astype(jnp.int32)
        + hub.astype(jnp.int32) * (nz * nc - 1)
        + has_next.astype(jnp.int32)
        + has_prev.astype(jnp.int32),
    )
    sent = []
    copies = border_copies(0, next_out0, prev_out0, from_prev0, from_next0)
    border_start(copies)
    lo_line = lax.broadcasted_iota(jnp.int32, (128, slots), 0).astype(F32).astype(BF16)
    hi_line = lax.broadcasted_iota(jnp.int32, (16, slots), 0).astype(F32).astype(BF16)
    one, none = jnp.ones((), BF16), jnp.zeros((), BF16)
    for c in range(cams):
        row = obs_ref[c : c + 1, :]
        low = (row & 127).astype(F32)
        high = (row >> 7).astype(F32)
        here = pl.ds(c * slots, slots)
        hit = jnp.where(spread(low, 128).astype(BF16) == lo_line, one, none)
        oh_lo2[:, here] = hit.astype(F8)
        oh_hi2[:, here] = jnp.where(spread(high, 16).astype(BF16) == hi_line, one if c % 2 == 0 else -one, none)

    precond = []
    for k in range(9):
        square = cj_ref[k].astype(F32) ** 2 + cj_ref[9 + k].astype(F32) ** 2
        precond.append(recip(cam_damp + narrow_sum(square * weights)))
    border_wait(copies)
    sent.append(copies)
    sums = [complete(sums[i], from_prev0[i], from_next0[i]) for i in range(9)]
    ent = sums[:6]
    cofactors = [
        ent[3] * ent[5] - ent[4] * ent[4],
        ent[2] * ent[4] - ent[1] * ent[5],
        ent[1] * ent[4] - ent[2] * ent[3],
        ent[0] * ent[5] - ent[2] * ent[2],
        ent[1] * ent[2] - ent[0] * ent[4],
        ent[0] * ent[3] - ent[1] * ent[1],
    ]
    determinant = ent[0] * cofactors[0] + ent[1] * cofactors[1] + ent[2] * cofactors[2]
    scale = recip(jnp.where(determinant > 0.0, determinant, 1.0))
    inverse = [member * scale for member in cofactors]
    image = finish(guess, errors, solve(sums[6:], inverse))
    res0 = [right[k] - image[k] for k in range(9)]
    dir0 = [precond[k] * res0[k] for k in range(9)]

    def forward(vector, index):
        errors = project(vector)
        products(0, errors)
        result = scatter_wide(3)
        sums = [
            result[32 * i : 32 * i + 16] + result[32 * i + 16 : 32 * i + 32] for i in range(3)
        ]
        to_next, to_prev = next_out.at[index], prev_out.at[index]
        for i in range(3):
            outgoing(sums[i], i, to_next, to_prev)
        copies = border_copies(
            1 + index, to_next, to_prev, from_prev.at[index], from_next.at[index]
        )
        border_start(copies)
        return errors, sums, copies

    def arrived(index, sums):
        return [complete(sums[i], from_prev[index, i], from_next[index, i]) for i in range(3)]

    lane = lax.broadcasted_iota(jnp.int32, (1, 128), 1)

    errors, sums, copies = forward(dir0, 0)
    border_wait(copies)
    sent.append(copies)
    sums = arrived(0, sums)
    img0 = finish(dir0, errors, solve(sums, inverse))
    res_t = [res0[k] - img0[k] for k in range(9)]
    dir_t = [precond[k] * res_t[k] for k in range(9)]
    errors, sums, copies = forward(dir_t, 1)
    scalars = [
        inner(res0, dir0),
        inner(dir0, img0),
        inner(res_t, dir0),
        inner(img0, dir_t),
        inner(res_t, dir_t),
    ]
    row = jnp.zeros((1, 128), F32)
    for i, scalar in enumerate(scalars):
        row = jnp.where(lane == i, scalar, row)
    damped = jnp.sum(cam_damp * sum(entry * entry for entry in dir_t), axis=0, keepdims=True)
    squares = errors[0] * errors[0] + errors[1] * errors[1]
    squares = jnp.sum(squares, axis=0, keepdims=True)
    squares = sum(squares[:, 128 * t : 128 * (t + 1)] for t in range(tiles))
    border_wait(copies)
    sent.append(copies)
    sums = arrived(1, sums)
    points = solve(sums, inverse)
    energy = sum(sums[j][:8] * points[j][:8] for j in range(3))
    squares = squares - jnp.sum(energy, axis=0, keepdims=True)
    curve_t = damped + jnp.sum(squares, axis=1, keepdims=True)
    reduce_start(jnp.where(lane == len(scalars), curve_t, row))
    img_t = finish(dir_t, errors, points)
    flat_rows = [
        jnp.concatenate([lie(entry) for entry in vector], axis=0)
        for vector in (guess, dir0, dir_t, res_t, img0, img_t)
    ]
    for i, block in enumerate(flat_rows):
        rows_ref[i] = block
    for copies in sent:
        border_sent(copies)
    row = reduce_finish()

    def at(index):
        picked = jnp.sum(jnp.where(lane == index, row, 0.0), axis=1, keepdims=True)
        return jnp.broadcast_to(picked, (1, 128))

    inner0, curve0, mixed_t, cross_t, inner_t, curve_t = [at(i) for i in range(6)]
    shift = mixed_t * recip(curve0)
    step0 = 1.0 + shift
    inner1 = inner_t - 2.0 * shift * cross_t + shift * shift * (curve0 - cross_t)
    curve1 = step0 * step0 * curve_t - 2.0 * shift * step0 * cross_t + shift * shift * curve0
    ratio = inner1 * recip(inner0)
    step1 = inner1 * recip(curve1 - ratio * inner1 * recip(step0))
    first_part = (step0 + step1 * (ratio - shift))[:, :cams]
    image_part = (shift + step1 * (ratio - shift))[:, :cams]
    second_part = (step1 * step0)[:, :cams]
    out_ref[0] = rows_ref[0] + first_part * rows_ref[1] + second_part * rows_ref[2]
    out_ref[1] = rows_ref[3] - image_part * rows_ref[4] - second_part * rows_ref[5]
    reduce_sent()


def local(dims, cam_jac, point_jac, obs_point, obs_count, back_list, front_list, point_damp,
          cam_damp, right_side, start_guess):
    cams, slots = obs_point.shape
    entries = cams * slots
    nx, nz, ny, nc = dims
    arrays = (
        cam_jac,
        point_jac,
        obs_point,
        obs_count.reshape(1, cams),
        back_list,
        front_list,
        point_damp.reshape(8, 128),
        cam_damp.reshape(1, cams),
        right_side,
        start_guess,
    )
    arrays = tuple(pltpu.with_memory_space_constraint(array, pltpu.HBM) for array in arrays)
    vmem = pl.BlockSpec(memory_space=pltpu.VMEM)
    shape = jax.ShapeDtypeStruct((2, *right_side.shape), F32)
    both = pl.pallas_call(
        functools.partial(kernel, dims),
        out_shape=shape,
        in_specs=[pl.BlockSpec(memory_space=pltpu.HBM)] * len(arrays),
        out_specs=vmem,
        scratch_shapes=[
            *[pltpu.VMEM(array.shape, array.dtype) for array in arrays],
            pltpu.SemaphoreType.DMA((len(arrays) + 2,)),
            pltpu.VMEM((256, entries), F8),
            pltpu.VMEM((16, entries), BF16),
            pltpu.VMEM((128, entries), F8),
            pltpu.VMEM((16, entries), BF16),
            pltpu.VMEM((18, cams, slots), F32),
            pltpu.VMEM((2, cams, slots), F32),
            pltpu.VMEM((cams, slots), F32),
            pltpu.VMEM((3, 16, 128), F32),
            pltpu.VMEM((6, 9, cams), F32),
            pltpu.VMEM((9, 8, 128), F32),
            pltpu.VMEM((9, 8, 128), F32),
            pltpu.VMEM((9, 8, 128), F32),
            pltpu.VMEM((9, 8, 128), F32),
            pltpu.VMEM((2, 3, 8, 128), F32),
            pltpu.VMEM((2, 3, 8, 128), F32),
            pltpu.VMEM((2, 3, 8, 128), F32),
            pltpu.VMEM((2, 3, 8, 128), F32),
            pltpu.VMEM((1, 128), F32),
            pltpu.VMEM((nx * ny * nc, 1, 128), F32),
            pltpu.VMEM((1, 128), F32),
            pltpu.VMEM((nz, 1, 128), F32),
            pltpu.SemaphoreType.DMA((3, 2)),
            pltpu.SemaphoreType.DMA((3, 2)),
            pltpu.SemaphoreType.DMA((nx * ny,)),
            pltpu.SemaphoreType.DMA((nx * ny * nc,)),
            pltpu.SemaphoreType.DMA((nz * nc,)),
            pltpu.SemaphoreType.DMA((nz,)),
        ],
        compiler_params=pltpu.CompilerParams(
            collective_id=0, has_side_effects=True, vmem_limit_bytes=48 * 1024 * 1024
        ),
    )(*arrays)
    return both[0], both[1]


def solution(mesh):
    seg = "seg"
    return jax.shard_map(
        functools.partial(local, DIMS),
        mesh=mesh,
        in_specs=(
            P(None, seg, None),
            P(None, seg, None),
            P(seg, None),
            P(seg),
            P(seg, None),
            P(seg, None),
            P(seg),
            P(seg),
            P(None, seg),
            P(None, seg),
        ),
        out_specs=(P(None, seg), P(None, seg)),
        check_vma=False,
    )
```

```python
import functools

import jax
import jax.numpy as jnp
from jax import lax
from jax.experimental import pallas as pl
from jax.experimental.pallas import tpu as pltpu
from jax.sharding import PartitionSpec as P

DIMS = (4, 8, 4, 2)
HUB = 1
PAIRS = ((0, 0), (0, 1), (0, 2), (1, 1), (1, 2), (2, 2))
F32 = jnp.float32
BF16 = jnp.bfloat16
F8 = jnp.float8_e4m3fn
MESH = pl.DeviceIdType.MESH


def spread(block, rows):
    return jnp.broadcast_to(block, (rows, block.shape[1]))


def lane_pick(row, index):
    return jnp.take_along_axis(row, index, axis=1, mode="promise_in_bounds")


def recip(value):
    first = 1.0 / value
    return first * (2.0 - value * first)


def kernel(
    dims,
    cj_hbm,
    pj_hbm,
    obs_hbm,
    cnt_hbm,
    back_hbm,
    front_hbm,
    damp_hbm,
    cdamp_hbm,
    rhs_hbm,
    guess_hbm,
    out_ref,
    cj_ref,
    pj_ref,
    obs_ref,
    cnt_ref,
    back_ref,
    front_ref,
    damp_ref,
    cdamp_ref,
    rhs_ref,
    guess_ref,
    load_sem,
    oh_lo,
    oh_hi,
    oh_lo2,
    oh_hi2,
    pieces,
    err,
    wts,
    table,
    rows_ref,
    next_out0,
    prev_out0,
    from_prev0,
    from_next0,
    next_out,
    prev_out,
    from_prev,
    from_next,
    first_out,
    first_in,
    second_out,
    second_in,
    ex_send,
    ex_recv,
    first_send,
    first_recv,
    second_send,
    second_recv,
):
    nx, nz, ny, nc = dims
    total = nx * nz * ny * nc
    arrivals = [
        (obs_hbm, obs_ref),
        (cnt_hbm, cnt_ref),
        (guess_hbm, guess_ref),
        (back_hbm, back_ref),
        (front_hbm, front_ref),
        (pj_hbm, pj_ref),
        *[(cj_hbm.at[pl.ds(6 * i, 6)], cj_ref.at[pl.ds(6 * i, 6)]) for i in range(3)],
        (damp_hbm, damp_ref),
        (cdamp_hbm, cdamp_ref),
        (rhs_hbm, rhs_ref),
    ]
    loads = [
        pltpu.make_async_copy(source, target, load_sem.at[i])
        for i, (source, target) in enumerate(arrivals)
    ]
    for load in loads:
        load.start()
    cams, slots = obs_ref.shape
    tiles = slots // 128
    me = lax.axis_index("seg")
    core = lax.rem(me, nc)
    y = lax.rem(me // nc, ny)
    z = lax.rem(me // (nc * ny), nz)
    x = me // (nc * ny * nz)

    def ident(px, pz, py, pc):
        return ((px * nz + pz) * ny + py) * nc + pc

    plane_size = nx * ny
    hub = core == HUB

    def plane_at(step, sign):
        px = lax.rem(x + (step // ny if sign > 0 else nx - step // ny), nx)
        py = lax.rem(y + (step % ny if sign > 0 else ny - step % ny), ny)
        return px, py

    def height_at(step, sign):
        return lax.rem(z + (step if sign > 0 else nz - step), nz)

    has_next, has_prev = me < total - 1, me > 0

    barrier = pltpu.get_barrier_semaphore()

    def greet(device):
        pl.semaphore_signal(barrier, inc=1, device_id=(device,), device_id_type=MESH)

    @pl.when(hub)
    def _():
        for step in range(plane_size):
            px, py = plane_at(step, -1)
            for pc in range(nc):
                if step or pc != HUB:
                    greet(ident(px, z, py, pc))

    for step in range(1, nz):
        greet(ident(x, height_at(step, -1), y, HUB))

    @pl.when(jnp.logical_not(hub))
    def _():
        greet(ident(x, z, y, HUB))

    @pl.when(has_next)
    def _():
        pl.semaphore_signal(barrier, inc=1, device_id=(me + 1,), device_id_type=MESH)

    @pl.when(has_prev)
    def _():
        pl.semaphore_signal(barrier, inc=1, device_id=(me - 1,), device_id_type=MESH)

    @pl.when(jnp.logical_not(has_prev))
    def _():
        from_prev0[...] = jnp.zeros_like(from_prev0)
        from_prev[...] = jnp.zeros_like(from_prev)

    @pl.when(jnp.logical_not(has_next))
    def _():
        from_next0[...] = jnp.zeros_like(from_next0)
        from_next[...] = jnp.zeros_like(from_next)

    def border_copies(index, to_next, to_prev, came_prev, came_next):
        ahead = pltpu.make_async_remote_copy(
            src_ref=to_next,
            dst_ref=came_prev,
            send_sem=ex_send.at[index, 0],
            recv_sem=ex_recv.at[index, 0],
            device_id=(jnp.minimum(me + 1, total - 1),),
            device_id_type=MESH,
        )
        behind = pltpu.make_async_remote_copy(
            src_ref=to_prev,
            dst_ref=came_next,
            send_sem=ex_send.at[index, 1],
            recv_sem=ex_recv.at[index, 1],
            device_id=(jnp.maximum(me - 1, 0),),
            device_id_type=MESH,
        )
        return ahead, behind

    def border_start(copies):
        ahead, behind = copies

        @pl.when(has_next)
        def _():
            ahead.start()

        @pl.when(has_prev)
        def _():
            behind.start()

    def border_wait(copies):
        ahead, behind = copies

        @pl.when(has_prev)
        def _():
            ahead.wait_recv()

        @pl.when(has_next)
        def _():
            behind.wait_recv()

    def border_sent(copies):
        ahead, behind = copies

        @pl.when(has_prev)
        def _():
            behind.wait_send()

        @pl.when(has_next)
        def _():
            ahead.wait_send()

    plane_me = (x * ny + y) * nc + core

    def first_copy(step, sender_core, slot):
        px, py = plane_at(step, 1)
        return pltpu.make_async_remote_copy(
            src_ref=first_out,
            dst_ref=first_in.at[slot],
            send_sem=first_send.at[step],
            recv_sem=first_recv.at[step * nc + sender_core],
            device_id=(ident(px, z, py, HUB),),
            device_id_type=MESH,
        )

    def second_copy(step, pc, slot):
        return pltpu.make_async_remote_copy(
            src_ref=second_out,
            dst_ref=second_in.at[slot],
            send_sem=second_send.at[step * nc + pc],
            recv_sem=second_recv.at[step],
            device_id=(ident(x, height_at(step, 1), y, pc),),
            device_id_type=MESH,
        )

    far_first = sorted(
        range(1, plane_size),
        key=lambda step: -(
            min(step // ny, nx - step // ny) + min(step % ny, ny - step % ny)
        ),
    )
    high_first = sorted(range(1, nz), key=lambda step: -min(step, nz - step))

    def tree(terms):
        while len(terms) > 1:
            terms = [sum(terms[i : i + 2]) for i in range(0, len(terms), 2)]
        return terms[0]

    def reduce_start(value):
        first_out[...] = value
        for step in far_first:
            first_copy(step, core, plane_me).start()

        @pl.when(hub)
        def _():
            first_in[plane_me] = value

        @pl.when(jnp.logical_not(hub))
        def _():
            first_copy(0, core, plane_me).start()

    def reduce_finish():
        @pl.when(hub)
        def _():
            for step in range(plane_size):
                px, py = plane_at(step, -1)
                for pc in range(nc):
                    if step or pc != HUB:
                        first_copy(step, pc, (px * ny + py) * nc + pc).wait_recv()
            value = tree([first_in[slot] for slot in range(plane_size * nc)])
            second_out[...] = value
            second_in[z] = value
            for step in high_first:
                for pc in range(nc):
                    second_copy(step, pc, z).start()
            for pc in range(nc):
                if pc != HUB:
                    second_copy(0, pc, z).start()

        @pl.when(jnp.logical_not(hub))
        def _():
            second_copy(0, core, z).wait_recv()

        for step in range(1, nz):
            second_copy(step, core, height_at(step, -1)).wait_recv()

        return tree([second_in[slot] for slot in range(nz)])

    def reduce_sent():
        for step in far_first:
            first_copy(step, core, plane_me).wait_send()

        @pl.when(jnp.logical_not(hub))
        def _():
            first_copy(0, core, plane_me).wait_send()

        @pl.when(hub)
        def _():
            for step in high_first:
                for pc in range(nc):
                    second_copy(step, pc, z).wait_send()
            for pc in range(nc):
                if pc != HUB:
                    second_copy(0, pc, z).wait_send()

    eye = lax.broadcasted_iota(jnp.int32, (cams, cams), 0) == lax.broadcasted_iota(
        jnp.int32, (cams, cams), 1
    )

    def stand(row):
        summed = jnp.sum(jnp.where(eye, spread(row, cams), 0.0), axis=1, keepdims=True)
        return jnp.broadcast_to(summed, (cams, 128))

    eye_wide = lax.broadcasted_iota(jnp.int32, (cams, 128), 0) == lax.broadcasted_iota(
        jnp.int32, (cams, 128), 1
    )

    def lie(block):
        return jnp.sum(jnp.where(eye_wide, block, 0.0), axis=0, keepdims=True)[:, :cams]

    def wide(block):
        return jnp.concatenate([block] * tiles, axis=1)

    def stack(block):
        return jnp.concatenate(
            [block[:, 128 * t : 128 * (t + 1)] for t in range(tiles)], axis=0
        )

    def narrow_sum(block):
        summed = jnp.sum(block, axis=1, keepdims=True)
        return jnp.broadcast_to(summed, (cams, 128))

    def inner(first, second):
        running = first[0] * second[0]
        for k in range(1, 9):
            running = running + first[k] * second[k]
        return jnp.sum(running, axis=0, keepdims=True)

    for load in loads:
        load.wait()
    count = stand(cnt_ref[...].astype(F32))
    guess = [stand(guess_ref[k : k + 1, :]) for k in range(9)]
    position = lax.broadcasted_iota(jnp.int32, (cams, slots), 1).astype(F32)
    wts[...] = jnp.where(position < wide(count), 1.0, 0.0)

    lo_line = lax.broadcasted_iota(jnp.int32, (256, slots), 0).astype(F32).astype(BF16)
    hi_line = lax.broadcasted_iota(jnp.int32, (16, slots), 0)
    hi_line = (hi_line & 7).astype(F32).astype(BF16)
    one, none = jnp.ones((), BF16), jnp.zeros((), BF16)
    for c in range(cams):
        row = obs_ref[c : c + 1, :]
        low = ((row & 127) + ((row >> 10) << 7)).astype(F32)
        high = ((row >> 7) & 7).astype(F32)
        here = pl.ds(c * slots, slots)
        hit = jnp.where(spread(low, 256).astype(BF16) == lo_line, one, none)
        oh_lo[:, here] = hit.astype(F8)
        oh_hi[:, here] = jnp.where(spread(high, 16).astype(BF16) == hi_line, one if c % 2 == 0 else -one, none)

    def scatter(values):
        halves = [None, None]
        for c in range(cams):
            here = pl.ds(c * slots, slots)
            mask = oh_hi[:, here]
            rows = []
            for v in range(values):
                pair = [spread(pieces[2 * v + p, c : c + 1, :], 8) for p in range(2)]
                rows.append(jnp.concatenate(pair, axis=0).astype(BF16) * mask)
            part = lax.dot_general(
                jnp.concatenate(rows, axis=0),
                oh_lo[:, here],
                (((1,), (1,)), ((), ())),
                preferred_element_type=F32,
            )
            before = halves[c % 2]
            halves[c % 2] = part if before is None else before + part
        return halves[0] - halves[1]

    def scatter_wide(values):
        halves = [None, None]
        for c in range(cams):
            here = pl.ds(c * slots, slots)
            mask = oh_hi2[:, here]
            rows = [
                spread(pieces[g, c : c + 1, :], 16).astype(BF16) * mask
                for g in range(2 * values)
            ]
            part = lax.dot_general(
                jnp.concatenate(rows, axis=0),
                oh_lo2[:, here],
                (((1,), (1,)), ((), ())),
                preferred_element_type=F32,
            )
            before = halves[c % 2]
            halves[c % 2] = part if before is None else before + part
        return halves[0] - halves[1]

    def cut(index, value):
        first = value.astype(BF16).astype(F32)
        pieces[2 * index] = first
        pieces[2 * index + 1] = value - first

    def joined(result, index):
        both = result[16 * index : 16 * index + 8] + result[16 * index + 8 : 16 * index + 16]
        return jnp.concatenate([both[:, :128], both[:, 128:]], axis=0)

    def project(vector):
        weights = wts[...]
        for row in range(2):
            running = cj_ref[9 * row].astype(F32) * wide(vector[0])
            for k in range(1, 9):
                running = running + cj_ref[9 * row + k].astype(F32) * wide(vector[k])
            err[row] = running * weights
        return err[0], err[1]

    def products(base, errors):
        for column_index in range(3):
            cut(
                base + column_index,
                errors[0] * pj_ref[column_index].astype(F32)
                + errors[1] * pj_ref[3 + column_index].astype(F32),
            )

    rows = [back_ref[:, 128 * t : 128 * (t + 1)] for t in range(3)]
    rows += [front_ref[:, 128 * t : 128 * (t + 1)] for t in range(3)]
    rows += [jnp.zeros((2, 128), jnp.int32)]
    listed = jnp.concatenate(rows, axis=0)
    list_lo, list_hi = listed & 127, listed >> 7
    flat = jnp.concatenate([back_ref[...], front_ref[...]], axis=1)
    width = flat.shape[1]
    flat_lo = spread((flat & 127).astype(F32), 128)
    flat_hi = spread((flat >> 7).astype(F32), 8)
    order = lax.broadcasted_iota(jnp.int32, (8, width), 1)
    hot_lo = jnp.where(
        flat_lo == lax.broadcasted_iota(jnp.int32, (128, width), 0).astype(F32), 1.0, 0.0
    ).astype(BF16)
    same_hi = flat_hi == lax.broadcasted_iota(jnp.int32, (8, width), 0).astype(F32)
    marks = jnp.concatenate(
        [
            jnp.where(same_hi, (order & 127).astype(F32), 0.0),
            jnp.where(same_hi, ((order >> 7) + 1).astype(F32), 0.0),
        ],
        axis=0,
    ).astype(BF16)
    places = lax.dot_general(
        marks, hot_lo, (((1,), (1,)), ((), ())), preferred_element_type=F32
    ).astype(jnp.int32)
    place_lo, place_hi = places[:8], places[8:16] - 1

    def choose(options, bits):
        for bit in bits:
            options = [
                jnp.where(bit, options[i + 1], options[i]) if i + 1 < len(options) else options[i]
                for i in range(0, len(options), 2)
            ]
        return options[0]

    list_bits = [(list_hi & (1 << b)) != 0 for b in range(3)]
    place_bits = [(place_hi & (1 << b)) != 0 for b in range(3)]
    sub8 = lax.broadcasted_iota(jnp.int32, (8, 128), 0)
    back_rows = sub8 < 3

    def outgoing(sums, index, to_next, to_prev):
        own, outer = sums[:8], sums[8:16]
        picked = choose(
            [lane_pick(spread(own[h : h + 1], 8), list_lo) for h in range(8)], list_bits
        )
        to_next[index] = jnp.where(back_rows, picked, outer)
        to_prev[index] = jnp.where(back_rows, outer, picked)

    def complete(sums, prev_block, next_block):
        own, outer = sums[:8], sums[8:16]
        mixed = jnp.where(back_rows, next_block, prev_block)
        added = choose(
            [lane_pick(spread(mixed[h : h + 1], 8), place_lo) for h in range(6)], place_bits
        )
        added = jnp.where(place_hi >= 0, added, 0.0)
        return jnp.concatenate(
            [own + added, outer + jnp.where(back_rows, prev_block, next_block)], axis=0
        )

    obs_lo, obs_hi = stack(obs_ref[...] & 127), stack(obs_ref[...] >> 7)

    def solve(sums, inverse):
        return [
            inverse[0] * sums[0] + inverse[1] * sums[1] + inverse[2] * sums[2],
            inverse[1] * sums[0] + inverse[3] * sums[1] + inverse[4] * sums[2],
            inverse[2] * sums[0] + inverse[4] * sums[1] + inverse[5] * sums[2],
        ]

    def finish(vector, errors, points):
        for j in range(3):
            table[j] = points[j]
        found = [[] for _ in range(3)]
        for block in range(cams * tiles // 8):
            low, high = (part[8 * block : 8 * block + 8] for part in (obs_lo, obs_hi))
            bits = [(high & (1 << b)) != 0 for b in range(4)]
            for j in range(3):
                found[j].append(
                    choose(
                        [lane_pick(spread(table[j, h : h + 1, :], 8), low) for h in range(14)],
                        bits,
                    )
                )
        picked = [
            jnp.concatenate(
                [
                    jnp.concatenate(found[j][cams // 8 * t : cams // 8 * (t + 1)], axis=0)
                    for t in range(tiles)
                ],
                axis=1,
            )
            for j in range(3)
        ]
        weights = wts[...]
        adjusted = []
        for row in range(2):
            term = picked[0] * pj_ref[3 * row].astype(F32)
            term = term + picked[1] * pj_ref[3 * row + 1].astype(F32)
            term = term + picked[2] * pj_ref[3 * row + 2].astype(F32)
            adjusted.append(errors[row] - weights * term)
        image = []
        for k in range(9):
            both = (
                cj_ref[k].astype(F32) * adjusted[0] + cj_ref[9 + k].astype(F32) * adjusted[1]
            )
            image.append(cam_damp * vector[k] + narrow_sum(both))
        return image

    cam_damp = stand(cdamp_ref[...])
    right = [stand(rhs_ref[k : k + 1, :]) for k in range(9)]

    errors = project(guess)
    weights = wts[...]
    for i, (a, b) in enumerate(PAIRS):
        product = pj_ref[a].astype(F32) * pj_ref[b].astype(F32)
        product = product + pj_ref[3 + a].astype(F32) * pj_ref[3 + b].astype(F32)
        cut(i, product * weights)
    products(6, errors)
    result = scatter(9)
    sums = []
    damping = jnp.concatenate([damp_ref[...], jnp.zeros((8, 128), F32)], axis=0)
    for i in range(9):
        value = joined(result, i)
        if i < 6 and PAIRS[i][0] == PAIRS[i][1]:
            value = value + damping
        outgoing(value, i, next_out0, prev_out0)
        sums.append(value)
    pl.semaphore_wait(
        barrier,
        plane_size
        - hub.astype(jnp.int32)
        + hub.astype(jnp.int32) * (nz * nc - 1)
        + has_next.astype(jnp.int32)
        + has_prev.astype(jnp.int32),
    )
    sent = []
    copies = border_copies(0, next_out0, prev_out0, from_prev0, from_next0)
    border_start(copies)
    lo_line = lax.broadcasted_iota(jnp.int32, (128, slots), 0).astype(F32).astype(BF16)
    hi_line = lax.broadcasted_iota(jnp.int32, (16, slots), 0).astype(F32).astype(BF16)
    one, none = jnp.ones((), BF16), jnp.zeros((), BF16)
    for c in range(cams):
        row = obs_ref[c : c + 1, :]
        low = (row & 127).astype(F32)
        high = (row >> 7).astype(F32)
        here = pl.ds(c * slots, slots)
        hit = jnp.where(spread(low, 128).astype(BF16) == lo_line, one, none)
        oh_lo2[:, here] = hit.astype(F8)
        oh_hi2[:, here] = jnp.where(spread(high, 16).astype(BF16) == hi_line, one if c % 2 == 0 else -one, none)

    precond = []
    for k in range(9):
        square = cj_ref[k].astype(F32) ** 2 + cj_ref[9 + k].astype(F32) ** 2
        precond.append(recip(cam_damp + narrow_sum(square * weights)))
    border_wait(copies)
    sent.append(copies)
    sums = [complete(sums[i], from_prev0[i], from_next0[i]) for i in range(9)]
    ent = sums[:6]
    cofactors = [
        ent[3] * ent[5] - ent[4] * ent[4],
        ent[2] * ent[4] - ent[1] * ent[5],
        ent[1] * ent[4] - ent[2] * ent[3],
        ent[0] * ent[5] - ent[2] * ent[2],
        ent[1] * ent[2] - ent[0] * ent[4],
        ent[0] * ent[3] - ent[1] * ent[1],
    ]
    determinant = ent[0] * cofactors[0] + ent[1] * cofactors[1] + ent[2] * cofactors[2]
    scale = recip(jnp.where(determinant > 0.0, determinant, 1.0))
    inverse = [member * scale for member in cofactors]
    image = finish(guess, errors, solve(sums[6:], inverse))
    res0 = [right[k] - image[k] for k in range(9)]
    dir0 = [precond[k] * res0[k] for k in range(9)]

    def forward(vector, index):
        errors = project(vector)
        products(0, errors)
        result = scatter_wide(3)
        sums = [
            result[32 * i : 32 * i + 16] + result[32 * i + 16 : 32 * i + 32] for i in range(3)
        ]
        to_next, to_prev = next_out.at[index], prev_out.at[index]
        for i in range(3):
            outgoing(sums[i], i, to_next, to_prev)
        copies = border_copies(
            1 + index, to_next, to_prev, from_prev.at[index], from_next.at[index]
        )
        border_start(copies)
        return errors, sums, copies

    def arrived(index, sums):
        return [complete(sums[i], from_prev[index, i], from_next[index, i]) for i in range(3)]

    lane = lax.broadcasted_iota(jnp.int32, (1, 128), 1)

    errors, sums, copies = forward(dir0, 0)
    border_wait(copies)
    sent.append(copies)
    sums = arrived(0, sums)
    img0 = finish(dir0, errors, solve(sums, inverse))
    res_t = [res0[k] - img0[k] for k in range(9)]
    dir_t = [precond[k] * res_t[k] for k in range(9)]
    errors, sums, copies = forward(dir_t, 1)
    scalars = [
        inner(res0, dir0),
        inner(dir0, img0),
        inner(res_t, dir0),
        inner(img0, dir_t),
        inner(res_t, dir_t),
    ]
    row = jnp.zeros((1, 128), F32)
    for i, scalar in enumerate(scalars):
        row = jnp.where(lane == i, scalar, row)
    damped = jnp.sum(cam_damp * sum(entry * entry for entry in dir_t), axis=0, keepdims=True)
    squares = errors[0] * errors[0] + errors[1] * errors[1]
    squares = jnp.sum(squares, axis=0, keepdims=True)
    squares = sum(squares[:, 128 * t : 128 * (t + 1)] for t in range(tiles))
    border_wait(copies)
    sent.append(copies)
    sums = arrived(1, sums)
    points = solve(sums, inverse)
    energy = sum(sums[j][:8] * points[j][:8] for j in range(3))
    squares = squares - jnp.sum(energy, axis=0, keepdims=True)
    curve_t = damped + jnp.sum(squares, axis=1, keepdims=True)
    reduce_start(jnp.where(lane == len(scalars), curve_t, row))
    img_t = finish(dir_t, errors, points)
    flat_rows = [
        jnp.concatenate([lie(entry) for entry in vector], axis=0)
        for vector in (guess, dir0, dir_t, res_t, img0, img_t)
    ]
    for i, block in enumerate(flat_rows):
        rows_ref[i] = block
    for copies in sent:
        border_sent(copies)
    row = reduce_finish()

    def at(index):
        picked = jnp.sum(jnp.where(lane == index, row, 0.0), axis=1, keepdims=True)
        return jnp.broadcast_to(picked, (1, 128))

    inner0, curve0, mixed_t, cross_t, inner_t, curve_t = [at(i) for i in range(6)]
    shift = mixed_t * recip(curve0)
    step0 = 1.0 + shift
    inner1 = inner_t - 2.0 * shift * cross_t + shift * shift * (curve0 - cross_t)
    curve1 = step0 * step0 * curve_t - 2.0 * shift * step0 * cross_t + shift * shift * curve0
    ratio = inner1 * recip(inner0)
    step1 = inner1 * recip(curve1 - ratio * inner1 * recip(step0))
    first_part = (step0 + step1 * (ratio - shift))[:, :cams]
    image_part = (shift + step1 * (ratio - shift))[:, :cams]
    second_part = (step1 * step0)[:, :cams]
    out_ref[0] = rows_ref[0] + first_part * rows_ref[1] + second_part * rows_ref[2]
    out_ref[1] = rows_ref[3] - image_part * rows_ref[4] - second_part * rows_ref[5]
    reduce_sent()


def local(dims, cam_jac, point_jac, obs_point, obs_count, back_list, front_list, point_damp,
          cam_damp, right_side, start_guess):
    cams, slots = obs_point.shape
    entries = cams * slots
    nx, nz, ny, nc = dims
    arrays = (
        cam_jac,
        point_jac,
        obs_point,
        obs_count.reshape(1, cams),
        back_list,
        front_list,
        point_damp.reshape(8, 128),
        cam_damp.reshape(1, cams),
        right_side,
        start_guess,
    )
    arrays = tuple(pltpu.with_memory_space_constraint(array, pltpu.HBM) for array in arrays)
    vmem = pl.BlockSpec(memory_space=pltpu.VMEM)
    shape = jax.ShapeDtypeStruct((2, *right_side.shape), F32)
    both = pl.pallas_call(
        functools.partial(kernel, dims),
        out_shape=shape,
        in_specs=[pl.BlockSpec(memory_space=pltpu.HBM)] * len(arrays),
        out_specs=vmem,
        scratch_shapes=[
            *[pltpu.VMEM(array.shape, array.dtype) for array in arrays],
            pltpu.SemaphoreType.DMA((len(arrays) + 2,)),
            pltpu.VMEM((256, entries), F8),
            pltpu.VMEM((16, entries), BF16),
            pltpu.VMEM((128, entries), F8),
            pltpu.VMEM((16, entries), BF16),
            pltpu.VMEM((18, cams, slots), F32),
            pltpu.VMEM((2, cams, slots), F32),
            pltpu.VMEM((cams, slots), F32),
            pltpu.VMEM((3, 16, 128), F32),
            pltpu.VMEM((6, 9, cams), F32),
            pltpu.VMEM((9, 8, 128), F32),
            pltpu.VMEM((9, 8, 128), F32),
            pltpu.VMEM((9, 8, 128), F32),
            pltpu.VMEM((9, 8, 128), F32),
            pltpu.VMEM((2, 3, 8, 128), F32),
            pltpu.VMEM((2, 3, 8, 128), F32),
            pltpu.VMEM((2, 3, 8, 128), F32),
            pltpu.VMEM((2, 3, 8, 128), F32),
            pltpu.VMEM((1, 128), F32),
            pltpu.VMEM((nx * ny * nc, 1, 128), F32),
            pltpu.VMEM((1, 128), F32),
            pltpu.VMEM((nz, 1, 128), F32),
            pltpu.SemaphoreType.DMA((3, 2)),
            pltpu.SemaphoreType.DMA((3, 2)),
            pltpu.SemaphoreType.DMA((nx * ny,)),
            pltpu.SemaphoreType.DMA((nx * ny * nc,)),
            pltpu.SemaphoreType.DMA((nz * nc,)),
            pltpu.SemaphoreType.DMA((nz,)),
        ],
        compiler_params=pltpu.CompilerParams(
            collective_id=0, has_side_effects=True, vmem_limit_bytes=48 * 1024 * 1024
        ),
    )(*arrays)
    return both[0], both[1]


def solution(mesh):
    seg = "seg"
    return jax.shard_map(
        functools.partial(local, DIMS),
        mesh=mesh,
        in_specs=(
            P(None, seg, None),
            P(None, seg, None),
            P(seg, None),
            P(seg),
            P(seg, None),
            P(seg, None),
            P(seg),
            P(seg),
            P(None, seg),
            P(None, seg),
        ),
        out_specs=(P(None, seg), P(None, seg)),
        check_vma=False,
    )
```

```python
import functools

import jax
import jax.numpy as jnp
from jax import lax
from jax.experimental import pallas as pl
from jax.experimental.pallas import tpu as pltpu
from jax.sharding import PartitionSpec as P

DIMS = (4, 8, 4, 2)
HUB = 1
PAIRS = ((0, 0), (0, 1), (0, 2), (1, 1), (1, 2), (2, 2))
F32 = jnp.float32
BF16 = jnp.bfloat16
F8 = jnp.float8_e4m3fn
MESH = pl.DeviceIdType.MESH


def spread(block, rows):
    return jnp.broadcast_to(block, (rows, block.shape[1]))


def lane_pick(row, index):
    return jnp.take_along_axis(row, index, axis=1, mode="promise_in_bounds")


def recip(value):
    first = 1.0 / value
    return first * (2.0 - value * first)


def kernel(
    dims,
    cj_hbm,
    pj_hbm,
    obs_hbm,
    cnt_hbm,
    back_hbm,
    front_hbm,
    damp_hbm,
    cdamp_hbm,
    rhs_hbm,
    guess_hbm,
    out_ref,
    cj_ref,
    pj_ref,
    obs_ref,
    cnt_ref,
    back_ref,
    front_ref,
    damp_ref,
    cdamp_ref,
    rhs_ref,
    guess_ref,
    load_sem,
    oh_lo,
    oh_hi,
    oh_lo2,
    oh_hi2,
    pieces,
    err,
    wts,
    table,
    rows_ref,
    next_out0,
    prev_out0,
    from_prev0,
    from_next0,
    next_out,
    prev_out,
    from_prev,
    from_next,
    first_out,
    first_in,
    second_out,
    second_in,
    ex_send,
    ex_recv,
    first_send,
    first_recv,
    second_send,
    second_recv,
):
    nx, nz, ny, nc = dims
    total = nx * nz * ny * nc
    arrivals = [
        (obs_hbm, obs_ref),
        (cnt_hbm, cnt_ref),
        (guess_hbm, guess_ref),
        (back_hbm, back_ref),
        (front_hbm, front_ref),
        (pj_hbm, pj_ref),
        *[(cj_hbm.at[pl.ds(6 * i, 6)], cj_ref.at[pl.ds(6 * i, 6)]) for i in range(3)],
        (damp_hbm, damp_ref),
        (cdamp_hbm, cdamp_ref),
        (rhs_hbm, rhs_ref),
    ]
    loads = [
        pltpu.make_async_copy(source, target, load_sem.at[i])
        for i, (source, target) in enumerate(arrivals)
    ]
    for load in loads:
        load.start()
    cams, slots = obs_ref.shape
    tiles = slots // 128
    me = lax.axis_index("seg")
    core = lax.rem(me, nc)
    y = lax.rem(me // nc, ny)
    z = lax.rem(me // (nc * ny), nz)
    x = me // (nc * ny * nz)

    def ident(px, pz, py, pc):
        return ((px * nz + pz) * ny + py) * nc + pc

    plane_size = nx * ny
    hub = core == HUB

    def plane_at(step, sign):
        px = lax.rem(x + (step // ny if sign > 0 else nx - step // ny), nx)
        py = lax.rem(y + (step % ny if sign > 0 else ny - step % ny), ny)
        return px, py

    def height_at(step, sign):
        return lax.rem(z + (step if sign > 0 else nz - step), nz)

    has_next, has_prev = me < total - 1, me > 0

    barrier = pltpu.get_barrier_semaphore()

    def greet(device):
        pl.semaphore_signal(barrier, inc=1, device_id=(device,), device_id_type=MESH)

    @pl.when(hub)
    def _():
        for step in range(plane_size):
            px, py = plane_at(step, -1)
            for pc in range(nc):
                if step or pc != HUB:
                    greet(ident(px, z, py, pc))

    for step in range(1, nz):
        greet(ident(x, height_at(step, -1), y, HUB))

    @pl.when(jnp.logical_not(hub))
    def _():
        greet(ident(x, z, y, HUB))

    @pl.when(has_next)
    def _():
        pl.semaphore_signal(barrier, inc=1, device_id=(me + 1,), device_id_type=MESH)

    @pl.when(has_prev)
    def _():
        pl.semaphore_signal(barrier, inc=1, device_id=(me - 1,), device_id_type=MESH)

    @pl.when(jnp.logical_not(has_prev))
    def _():
        from_prev0[...] = jnp.zeros_like(from_prev0)
        from_prev[...] = jnp.zeros_like(from_prev)

    @pl.when(jnp.logical_not(has_next))
    def _():
        from_next0[...] = jnp.zeros_like(from_next0)
        from_next[...] = jnp.zeros_like(from_next)

    def border_copies(index, to_next, to_prev, came_prev, came_next):
        ahead = pltpu.make_async_remote_copy(
            src_ref=to_next.at[:, pl.ds(0, 6)],
            dst_ref=came_prev.at[:, pl.ds(0, 6)],
            send_sem=ex_send.at[index, 0],
            recv_sem=ex_recv.at[index, 0],
            device_id=(jnp.minimum(me + 1, total - 1),),
            device_id_type=MESH,
        )
        behind = pltpu.make_async_remote_copy(
            src_ref=to_prev.at[:, pl.ds(0, 6)],
            dst_ref=came_next.at[:, pl.ds(0, 6)],
            send_sem=ex_send.at[index, 1],
            recv_sem=ex_recv.at[index, 1],
            device_id=(jnp.maximum(me - 1, 0),),
            device_id_type=MESH,
        )
        return ahead, behind

    def border_start(copies):
        ahead, behind = copies

        @pl.when(has_next)
        def _():
            ahead.start()

        @pl.when(has_prev)
        def _():
            behind.start()

    def border_wait(copies):
        ahead, behind = copies

        @pl.when(has_prev)
        def _():
            ahead.wait_recv()

        @pl.when(has_next)
        def _():
            behind.wait_recv()

    def border_sent(copies):
        ahead, behind = copies

        @pl.when(has_prev)
        def _():
            behind.wait_send()

        @pl.when(has_next)
        def _():
            ahead.wait_send()

    plane_me = (x * ny + y) * nc + core

    def first_copy(step, sender_core, slot):
        px, py = plane_at(step, 1)
        return pltpu.make_async_remote_copy(
            src_ref=first_out,
            dst_ref=first_in.at[slot],
            send_sem=first_send.at[step],
            recv_sem=first_recv.at[step * nc + sender_core],
            device_id=(ident(px, z, py, HUB),),
            device_id_type=MESH,
        )

    def second_copy(step, pc, slot):
        return pltpu.make_async_remote_copy(
            src_ref=second_out,
            dst_ref=second_in.at[slot],
            send_sem=second_send.at[step * nc + pc],
            recv_sem=second_recv.at[step],
            device_id=(ident(x, height_at(step, 1), y, pc),),
            device_id_type=MESH,
        )

    far_first = sorted(
        range(1, plane_size),
        key=lambda step: -(
            min(step // ny, nx - step // ny) + min(step % ny, ny - step % ny)
        ),
    )
    high_first = sorted(range(1, nz), key=lambda step: -min(step, nz - step))

    def tree(terms):
        while len(terms) > 1:
            terms = [sum(terms[i : i + 2]) for i in range(0, len(terms), 2)]
        return terms[0]

    def reduce_start(value):
        first_out[...] = value
        for step in far_first:
            first_copy(step, core, plane_me).start()

        @pl.when(hub)
        def _():
            first_in[plane_me] = value

        @pl.when(jnp.logical_not(hub))
        def _():
            first_copy(0, core, plane_me).start()

    def reduce_finish():
        @pl.when(hub)
        def _():
            for step in range(plane_size):
                px, py = plane_at(step, -1)
                for pc in range(nc):
                    if step or pc != HUB:
                        first_copy(step, pc, (px * ny + py) * nc + pc).wait_recv()
            value = tree([first_in[slot] for slot in range(plane_size * nc)])
            second_out[...] = value
            second_in[z] = value
            for step in high_first:
                for pc in range(nc):
                    second_copy(step, pc, z).start()
            for pc in range(nc):
                if pc != HUB:
                    second_copy(0, pc, z).start()

        @pl.when(jnp.logical_not(hub))
        def _():
            second_copy(0, core, z).wait_recv()

        for step in range(1, nz):
            second_copy(step, core, height_at(step, -1)).wait_recv()

        return tree([second_in[slot] for slot in range(nz)])

    def reduce_sent():
        for step in far_first:
            first_copy(step, core, plane_me).wait_send()

        @pl.when(jnp.logical_not(hub))
        def _():
            first_copy(0, core, plane_me).wait_send()

        @pl.when(hub)
        def _():
            for step in high_first:
                for pc in range(nc):
                    second_copy(step, pc, z).wait_send()
            for pc in range(nc):
                if pc != HUB:
                    second_copy(0, pc, z).wait_send()

    eye = lax.broadcasted_iota(jnp.int32, (cams, cams), 0) == lax.broadcasted_iota(
        jnp.int32, (cams, cams), 1
    )

    def stand(row):
        summed = jnp.sum(jnp.where(eye, spread(row, cams), 0.0), axis=1, keepdims=True)
        return jnp.broadcast_to(summed, (cams, 128))

    eye_wide = lax.broadcasted_iota(jnp.int32, (cams, 128), 0) == lax.broadcasted_iota(
        jnp.int32, (cams, 128), 1
    )

    def lie(block):
        return jnp.sum(jnp.where(eye_wide, block, 0.0), axis=0, keepdims=True)[:, :cams]

    def wide(block):
        return jnp.concatenate([block] * tiles, axis=1)

    def stack(block):
        return jnp.concatenate(
            [block[:, 128 * t : 128 * (t + 1)] for t in range(tiles)], axis=0
        )

    def narrow_sum(block):
        summed = jnp.sum(block, axis=1, keepdims=True)
        return jnp.broadcast_to(summed, (cams, 128))

    def inner(first, second):
        running = first[0] * second[0]
        for k in range(1, 9):
            running = running + first[k] * second[k]
        return jnp.sum(running, axis=0, keepdims=True)

    for load in loads:
        load.wait()
    count = stand(cnt_ref[...].astype(F32))
    guess = [stand(guess_ref[k : k + 1, :]) for k in range(9)]
    position = lax.broadcasted_iota(jnp.int32, (cams, slots), 1).astype(F32)
    wts[...] = jnp.where(position < wide(count), 1.0, 0.0)

    lo_line = lax.broadcasted_iota(jnp.int32, (256, slots), 0).astype(F32).astype(BF16)
    hi_line = lax.broadcasted_iota(jnp.int32, (16, slots), 0)
    hi_line = (hi_line & 7).astype(F32).astype(BF16)
    one, none = jnp.ones((), BF16), jnp.zeros((), BF16)
    for c in range(cams):
        row = obs_ref[c : c + 1, :]
        low = ((row & 127) + ((row >> 10) << 7)).astype(F32)
        high = ((row >> 7) & 7).astype(F32)
        here = pl.ds(c * slots, slots)
        hit = jnp.where(spread(low, 256).astype(BF16) == lo_line, one, none)
        oh_lo[:, here] = hit.astype(F8)
        oh_hi[:, here] = jnp.where(spread(high, 16).astype(BF16) == hi_line, one if c % 2 == 0 else -one, none)

    def scatter(values):
        halves = [None, None]
        for c in range(cams):
            here = pl.ds(c * slots, slots)
            mask = oh_hi[:, here]
            rows = []
            for v in range(values):
                pair = [spread(pieces[2 * v + p, c : c + 1, :], 8) for p in range(2)]
                rows.append(jnp.concatenate(pair, axis=0).astype(BF16) * mask)
            part = lax.dot_general(
                jnp.concatenate(rows, axis=0),
                oh_lo[:, here],
                (((1,), (1,)), ((), ())),
                preferred_element_type=F32,
            )
            before = halves[c % 2]
            halves[c % 2] = part if before is None else before + part
        return halves[0] - halves[1]

    def scatter_wide(values):
        halves = [None, None]
        for c in range(cams):
            here = pl.ds(c * slots, slots)
            mask = oh_hi2[:, here]
            rows = [
                spread(pieces[g, c : c + 1, :], 16).astype(BF16) * mask
                for g in range(2 * values)
            ]
            part = lax.dot_general(
                jnp.concatenate(rows, axis=0),
                oh_lo2[:, here],
                (((1,), (1,)), ((), ())),
                preferred_element_type=F32,
            )
            before = halves[c % 2]
            halves[c % 2] = part if before is None else before + part
        return halves[0] - halves[1]

    def cut(index, value):
        first = value.astype(BF16).astype(F32)
        pieces[2 * index] = first
        pieces[2 * index + 1] = value - first

    def joined(result, index):
        both = result[16 * index : 16 * index + 8] + result[16 * index + 8 : 16 * index + 16]
        return jnp.concatenate([both[:, :128], both[:, 128:]], axis=0)

    def project(vector):
        weights = wts[...]
        for row in range(2):
            running = cj_ref[9 * row].astype(F32) * wide(vector[0])
            for k in range(1, 9):
                running = running + cj_ref[9 * row + k].astype(F32) * wide(vector[k])
            err[row] = running * weights
        return err[0], err[1]

    def products(base, errors):
        for column_index in range(3):
            cut(
                base + column_index,
                errors[0] * pj_ref[column_index].astype(F32)
                + errors[1] * pj_ref[3 + column_index].astype(F32),
            )

    rows = [back_ref[:, 128 * t : 128 * (t + 1)] for t in range(3)]
    rows += [front_ref[:, 128 * t : 128 * (t + 1)] for t in range(3)]
    rows += [jnp.zeros((2, 128), jnp.int32)]
    listed = jnp.concatenate(rows, axis=0)
    list_lo, list_hi = listed & 127, listed >> 7
    flat = jnp.concatenate([back_ref[...], front_ref[...]], axis=1)
    width = flat.shape[1]
    flat_lo = spread((flat & 127).astype(F32), 128)
    flat_hi = spread((flat >> 7).astype(F32), 8)
    order = lax.broadcasted_iota(jnp.int32, (8, width), 1)
    hot_lo = jnp.where(
        flat_lo == lax.broadcasted_iota(jnp.int32, (128, width), 0).astype(F32), 1.0, 0.0
    ).astype(BF16)
    same_hi = flat_hi == lax.broadcasted_iota(jnp.int32, (8, width), 0).astype(F32)
    marks = jnp.concatenate(
        [
            jnp.where(same_hi, (order & 127).astype(F32), 0.0),
            jnp.where(same_hi, ((order >> 7) + 1).astype(F32), 0.0),
        ],
        axis=0,
    ).astype(BF16)
    places = lax.dot_general(
        marks, hot_lo, (((1,), (1,)), ((), ())), preferred_element_type=F32
    ).astype(jnp.int32)
    place_lo, place_hi = places[:8], places[8:16] - 1

    def choose(options, bits):
        for bit in bits:
            options = [
                jnp.where(bit, options[i + 1], options[i]) if i + 1 < len(options) else options[i]
                for i in range(0, len(options), 2)
            ]
        return options[0]

    list_bits = [(list_hi & (1 << b)) != 0 for b in range(3)]
    place_bits = [(place_hi & (1 << b)) != 0 for b in range(3)]
    sub8 = lax.broadcasted_iota(jnp.int32, (8, 128), 0)
    back_rows = sub8 < 3

    def outgoing(sums, index, to_next, to_prev):
        own, outer = sums[:8], sums[8:16]
        picked = choose(
            [lane_pick(spread(own[h : h + 1], 8), list_lo) for h in range(8)], list_bits
        )
        to_next[index] = jnp.where(back_rows, picked, outer)
        to_prev[index] = jnp.where(back_rows, outer, picked)

    def complete(sums, prev_block, next_block):
        own, outer = sums[:8], sums[8:16]
        prev_block = jnp.where(sub8 < 6, prev_block, 0.0)
        next_block = jnp.where(sub8 < 6, next_block, 0.0)
        mixed = jnp.where(back_rows, next_block, prev_block)
        added = choose(
            [lane_pick(spread(mixed[h : h + 1], 8), place_lo) for h in range(6)], place_bits
        )
        added = jnp.where(place_hi >= 0, added, 0.0)
        return jnp.concatenate(
            [own + added, outer + jnp.where(back_rows, prev_block, next_block)], axis=0
        )

    obs_lo, obs_hi = stack(obs_ref[...] & 127), stack(obs_ref[...] >> 7)

    def solve(sums, inverse):
        return [
            inverse[0] * sums[0] + inverse[1] * sums[1] + inverse[2] * sums[2],
            inverse[1] * sums[0] + inverse[3] * sums[1] + inverse[4] * sums[2],
            inverse[2] * sums[0] + inverse[4] * sums[1] + inverse[5] * sums[2],
        ]

    def finish(vector, errors, points):
        for j in range(3):
            table[j] = points[j]
        found = [[] for _ in range(3)]
        for block in range(cams * tiles // 8):
            low, high = (part[8 * block : 8 * block + 8] for part in (obs_lo, obs_hi))
            bits = [(high & (1 << b)) != 0 for b in range(4)]
            for j in range(3):
                found[j].append(
                    choose(
                        [lane_pick(spread(table[j, h : h + 1, :], 8), low) for h in range(14)],
                        bits,
                    )
                )
        picked = [
            jnp.concatenate(
                [
                    jnp.concatenate(found[j][cams // 8 * t : cams // 8 * (t + 1)], axis=0)
                    for t in range(tiles)
                ],
                axis=1,
            )
            for j in range(3)
        ]
        weights = wts[...]
        adjusted = []
        for row in range(2):
            term = picked[0] * pj_ref[3 * row].astype(F32)
            term = term + picked[1] * pj_ref[3 * row + 1].astype(F32)
            term = term + picked[2] * pj_ref[3 * row + 2].astype(F32)
            adjusted.append(errors[row] - weights * term)
        image = []
        for k in range(9):
            both = (
                cj_ref[k].astype(F32) * adjusted[0] + cj_ref[9 + k].astype(F32) * adjusted[1]
            )
            image.append(cam_damp * vector[k] + narrow_sum(both))
        return image

    cam_damp = stand(cdamp_ref[...])
    right = [stand(rhs_ref[k : k + 1, :]) for k in range(9)]

    errors = project(guess)
    weights = wts[...]
    for i, (a, b) in enumerate(PAIRS):
        product = pj_ref[a].astype(F32) * pj_ref[b].astype(F32)
        product = product + pj_ref[3 + a].astype(F32) * pj_ref[3 + b].astype(F32)
        cut(i, product * weights)
    products(6, errors)
    result = scatter(9)
    sums = []
    damping = jnp.concatenate([damp_ref[...], jnp.zeros((8, 128), F32)], axis=0)
    for i in range(9):
        value = joined(result, i)
        if i < 6 and PAIRS[i][0] == PAIRS[i][1]:
            value = value + damping
        outgoing(value, i, next_out0, prev_out0)
        sums.append(value)
    pl.semaphore_wait(
        barrier,
        plane_size
        - hub.astype(jnp.int32)
        + hub.astype(jnp.int32) * (nz * nc - 1)
        + has_next.astype(jnp.int32)
        + has_prev.astype(jnp.int32),
    )
    sent = []
    copies = border_copies(0, next_out0, prev_out0, from_prev0, from_next0)
    border_start(copies)
    lo_line = lax.broadcasted_iota(jnp.int32, (128, slots), 0).astype(F32).astype(BF16)
    hi_line = lax.broadcasted_iota(jnp.int32, (16, slots), 0).astype(F32).astype(BF16)
    one, none = jnp.ones((), BF16), jnp.zeros((), BF16)
    for c in range(cams):
        row = obs_ref[c : c + 1, :]
        low = (row & 127).astype(F32)
        high = (row >> 7).astype(F32)
        here = pl.ds(c * slots, slots)
        hit = jnp.where(spread(low, 128).astype(BF16) == lo_line, one, none)
        oh_lo2[:, here] = hit.astype(F8)
        oh_hi2[:, here] = jnp.where(spread(high, 16).astype(BF16) == hi_line, one if c % 2 == 0 else -one, none)

    precond = []
    for k in range(9):
        square = cj_ref[k].astype(F32) ** 2 + cj_ref[9 + k].astype(F32) ** 2
        precond.append(recip(cam_damp + narrow_sum(square * weights)))
    border_wait(copies)
    sent.append(copies)
    sums = [complete(sums[i], from_prev0[i], from_next0[i]) for i in range(9)]
    ent = sums[:6]
    cofactors = [
        ent[3] * ent[5] - ent[4] * ent[4],
        ent[2] * ent[4] - ent[1] * ent[5],
        ent[1] * ent[4] - ent[2] * ent[3],
        ent[0] * ent[5] - ent[2] * ent[2],
        ent[1] * ent[2] - ent[0] * ent[4],
        ent[0] * ent[3] - ent[1] * ent[1],
    ]
    determinant = ent[0] * cofactors[0] + ent[1] * cofactors[1] + ent[2] * cofactors[2]
    scale = recip(jnp.where(determinant > 0.0, determinant, 1.0))
    inverse = [member * scale for member in cofactors]
    image = finish(guess, errors, solve(sums[6:], inverse))
    res0 = [right[k] - image[k] for k in range(9)]
    dir0 = [precond[k] * res0[k] for k in range(9)]

    def forward(vector, index):
        errors = project(vector)
        products(0, errors)
        result = scatter_wide(3)
        sums = [
            result[32 * i : 32 * i + 16] + result[32 * i + 16 : 32 * i + 32] for i in range(3)
        ]
        to_next, to_prev = next_out.at[index], prev_out.at[index]
        for i in range(3):
            outgoing(sums[i], i, to_next, to_prev)
        copies = border_copies(
            1 + index, to_next, to_prev, from_prev.at[index], from_next.at[index]
        )
        border_start(copies)
        return errors, sums, copies

    def arrived(index, sums):
        return [complete(sums[i], from_prev[index, i], from_next[index, i]) for i in range(3)]

    lane = lax.broadcasted_iota(jnp.int32, (1, 128), 1)

    errors, sums, copies = forward(dir0, 0)
    border_wait(copies)
    sent.append(copies)
    sums = arrived(0, sums)
    img0 = finish(dir0, errors, solve(sums, inverse))
    res_t = [res0[k] - img0[k] for k in range(9)]
    dir_t = [precond[k] * res_t[k] for k in range(9)]
    errors, sums, copies = forward(dir_t, 1)
    scalars = [
        inner(res0, dir0),
        inner(dir0, img0),
        inner(res_t, dir0),
        inner(img0, dir_t),
        inner(res_t, dir_t),
    ]
    row = jnp.zeros((1, 128), F32)
    for i, scalar in enumerate(scalars):
        row = jnp.where(lane == i, scalar, row)
    damped = jnp.sum(cam_damp * sum(entry * entry for entry in dir_t), axis=0, keepdims=True)
    squares = errors[0] * errors[0] + errors[1] * errors[1]
    squares = jnp.sum(squares, axis=0, keepdims=True)
    squares = sum(squares[:, 128 * t : 128 * (t + 1)] for t in range(tiles))
    border_wait(copies)
    sent.append(copies)
    sums = arrived(1, sums)
    points = solve(sums, inverse)
    energy = sum(sums[j][:8] * points[j][:8] for j in range(3))
    squares = squares - jnp.sum(energy, axis=0, keepdims=True)
    curve_t = damped + jnp.sum(squares, axis=1, keepdims=True)
    reduce_start(jnp.where(lane == len(scalars), curve_t, row))
    img_t = finish(dir_t, errors, points)
    flat_rows = [
        jnp.concatenate([lie(entry) for entry in vector], axis=0)
        for vector in (guess, dir0, dir_t, res_t, img0, img_t)
    ]
    for i, block in enumerate(flat_rows):
        rows_ref[i] = block
    for copies in sent:
        border_sent(copies)
    row = reduce_finish()

    def at(index):
        picked = jnp.sum(jnp.where(lane == index, row, 0.0), axis=1, keepdims=True)
        return jnp.broadcast_to(picked, (1, 128))

    inner0, curve0, mixed_t, cross_t, inner_t, curve_t = [at(i) for i in range(6)]
    shift = mixed_t * recip(curve0)
    step0 = 1.0 + shift
    inner1 = inner_t - 2.0 * shift * cross_t + shift * shift * (curve0 - cross_t)
    curve1 = step0 * step0 * curve_t - 2.0 * shift * step0 * cross_t + shift * shift * curve0
    ratio = inner1 * recip(inner0)
    step1 = inner1 * recip(curve1 - ratio * inner1 * (curve0 * recip(curve0 + mixed_t)))
    first_part = (step0 + step1 * (ratio - shift))[:, :cams]
    image_part = (shift + step1 * (ratio - shift))[:, :cams]
    second_part = (step1 * step0)[:, :cams]
    out_ref[0] = rows_ref[0] + first_part * rows_ref[1] + second_part * rows_ref[2]
    out_ref[1] = rows_ref[3] - image_part * rows_ref[4] - second_part * rows_ref[5]
    reduce_sent()


def local(dims, cam_jac, point_jac, obs_point, obs_count, back_list, front_list, point_damp,
          cam_damp, right_side, start_guess):
    cams, slots = obs_point.shape
    entries = cams * slots
    nx, nz, ny, nc = dims
    arrays = (
        cam_jac,
        point_jac,
        obs_point,
        obs_count.reshape(1, cams),
        back_list,
        front_list,
        point_damp.reshape(8, 128),
        cam_damp.reshape(1, cams),
        right_side,
        start_guess,
    )
    arrays = tuple(pltpu.with_memory_space_constraint(array, pltpu.HBM) for array in arrays)
    vmem = pl.BlockSpec(memory_space=pltpu.VMEM)
    shape = jax.ShapeDtypeStruct((2, *right_side.shape), F32)
    both = pl.pallas_call(
        functools.partial(kernel, dims),
        out_shape=shape,
        in_specs=[pl.BlockSpec(memory_space=pltpu.HBM)] * len(arrays),
        out_specs=vmem,
        scratch_shapes=[
            *[pltpu.VMEM(array.shape, array.dtype) for array in arrays],
            pltpu.SemaphoreType.DMA((len(arrays) + 2,)),
            pltpu.VMEM((256, entries), F8),
            pltpu.VMEM((16, entries), BF16),
            pltpu.VMEM((128, entries), F8),
            pltpu.VMEM((16, entries), BF16),
            pltpu.VMEM((18, cams, slots), F32),
            pltpu.VMEM((2, cams, slots), F32),
            pltpu.VMEM((cams, slots), F32),
            pltpu.VMEM((3, 16, 128), F32),
            pltpu.VMEM((6, 9, cams), F32),
            pltpu.VMEM((9, 8, 128), F32),
            pltpu.VMEM((9, 8, 128), F32),
            pltpu.VMEM((9, 8, 128), F32),
            pltpu.VMEM((9, 8, 128), F32),
            pltpu.VMEM((2, 3, 8, 128), F32),
            pltpu.VMEM((2, 3, 8, 128), F32),
            pltpu.VMEM((2, 3, 8, 128), F32),
            pltpu.VMEM((2, 3, 8, 128), F32),
            pltpu.VMEM((1, 128), F32),
            pltpu.VMEM((nx * ny * nc, 1, 128), F32),
            pltpu.VMEM((1, 128), F32),
            pltpu.VMEM((nz, 1, 128), F32),
            pltpu.SemaphoreType.DMA((3, 2)),
            pltpu.SemaphoreType.DMA((3, 2)),
            pltpu.SemaphoreType.DMA((nx * ny,)),
            pltpu.SemaphoreType.DMA((nx * ny * nc,)),
            pltpu.SemaphoreType.DMA((nz * nc,)),
            pltpu.SemaphoreType.DMA((nz,)),
        ],
        compiler_params=pltpu.CompilerParams(
            collective_id=0, has_side_effects=True, vmem_limit_bytes=48 * 1024 * 1024
        ),
    )(*arrays)
    return both[0], both[1]


def solution(mesh):
    seg = "seg"
    return jax.shard_map(
        functools.partial(local, DIMS),
        mesh=mesh,
        in_specs=(
            P(None, seg, None),
            P(None, seg, None),
            P(seg, None),
            P(seg),
            P(seg, None),
            P(seg, None),
            P(seg),
            P(seg),
            P(None, seg),
            P(None, seg),
        ),
        out_specs=(P(None, seg), P(None, seg)),
        check_vma=False,
    )
```
